1024 devices in a mesh: gx: 128 (over y_hi, z, core), gz: 8 (over x, y_lo).
Axes of the slice: x: 4, y: 8 (y_hi: 4, y_lo: 2; y = y_hi * 2 + y_lo), z: 16, core: 2. Of those that a mesh axis runs over, the one named last changes fastest.
Arguments:
- state: float32 [256, 16, 5, 12, 216], P('gx', 'gz'), as said below
- register: float32 [256, 16, 5, 12, 216], P('gx', 'gz'), may hold values from -6 to 6
- heights: float32 [12], replicated, may hold values from 0.05 to 0.3
- solid_wall_mask: int32 [256, 16, 11], P('gx', 'gz'), may hold values 0 or 1
Outputs:
- state_next: float32 [256, 16, 5, 12, 216], P('gx', 'gz')
- register_next: float32 [256, 16, 5, 12, 216], P('gx', 'gz')
The draws below stay inside these ranges and needn't reach their ends.
Inputs may be any that keep to these rules, and one draw needn't show every extreme that they name: `state`: at every node the density lies in [0.5, 1.6], each velocity component in [-1.8, 1.8] and the pressure 0.4 (E - |m|^2 / (2 rho)) in [0.4, 2.0].
All inputs are finite; a program needn't handle non-finite values. No bound on the sum of `solid_wall_mask` on one device may be relied on, other than what follows from the above.
Results may differ from the reference program's by a relative error of at most 0.0003.
Values sent between devices are 32-bit elements; how exact they have to be, the bound alone decides.
No kernel may reach another device: no remote copies, remote signals or barrier semaphores. Data moves between devices by JAX's collectives and lax.ppermute only.
A program may use at most 64 MiB of HBM per device.

```python
import math
import jax
import jax.numpy as jnp
import numpy as np
from jax import lax

EX = 2
ELEMENTS_ACROSS = 12
ELEMENT_NODES = 216
STREAMWISE_COLS = 256
SPANWISE_COLS = 16


def draw_state(key, part):
    keys = jax.random.split(jax.random.fold_in(key, 17), 3)
    array_shape = (STREAMWISE_COLS, SPANWISE_COLS, ELEMENTS_ACROSS, ELEMENT_NODES)
    density = jax.random.uniform(keys[0], array_shape, jnp.float32, 0.7, 1.3)
    velocity = jnp.clip(0.7 * jax.random.normal(keys[1], (3,) + array_shape, jnp.float32), -1.8, 1.8)
    pressure = jax.random.uniform(keys[2], array_shape, jnp.float32, 0.6, 1.4)
    momentum = density[None] * velocity
    energy = pressure / 0.4 + 0.5 * density * jnp.sum(velocity * velocity, axis=0)
    return jnp.stack([density, momentum[0], momentum[1], momentum[2], energy], axis=2)


def place_ends(drawn, own_key, least, largest):
    longest = drawn.shape.index(max(drawn.shape))
    spots = []
    for shift in (0, 1):
        where = [jax.random.randint(jax.random.fold_in(own_key, axis), (), 0, length) for axis, length in enumerate(drawn.shape)]
        where[longest] = (where[longest] + shift) % drawn.shape[longest]
        spots.append(tuple(where))
    return drawn.at[spots[0]].set(least).at[spots[1]].set(largest)


def block_levels(key, dims, cuts, least, largest):
    def one(axis_at, shards_of):
        draws = jax.random.uniform(jax.random.fold_in(jax.random.fold_in(key, 6), axis_at), (shards_of,), jnp.float32, least / len(cuts), largest / len(cuts))
        return jnp.repeat(jnp.exp(draws), dims[axis_at] // shards_of).reshape((-1,) + (1,) * (len(dims) - axis_at - 1))

    factor_of = one(*cuts[0])
    for cut in cuts[1:]:
        factor_of = factor_of * one(*cut)
    return factor_of


def scatter_about(own_key, dims, deviation, reach, cuts=(), kind=jnp.bfloat16):
    loudness = block_levels(own_key, dims, cuts, -0.22, 0.18) if cuts else 1.0
    entries = jax.random.normal(own_key, dims, jnp.float32) * deviation * loudness
    return jnp.minimum(jnp.maximum(entries, -reach), reach).astype(kind)


def setup_inputs(seed: int = 0) -> dict:
    key_list = jax.random.split(jax.random.key(seed), 5)
    return {
        "state": draw_state(jax.random.fold_in(key_list[4], 71), 0),
        "register": scatter_about(key_list[1], (STREAMWISE_COLS, SPANWISE_COLS, 5, ELEMENTS_ACROSS, ELEMENT_NODES), 1.0, 6.0, ((0, 128), (1, 8)), jnp.float32),
        "heights": jnp.clip(jnp.exp(jax.random.uniform(key_list[2], (ELEMENTS_ACROSS,), jnp.float32, math.log(0.05), math.log(0.3))), 0.05, 0.3),
        "solid_wall_mask": place_ends((jax.random.randint(key_list[3], (STREAMWISE_COLS, SPANWISE_COLS, ELEMENTS_ACROSS - 1), 0, 6) < 1).astype(jnp.int32), jax.random.fold_in(key_list[3], 1), 0, 1),
    }


GAMMA = 1.4
VISCOSITY = 0.001
CONDUCT = 0.001 * 1.4 / (0.4 * 0.72)
LENGTH_X = 0.2
LENGTH_Z = 0.15
TIME_STEP = 0.004
SECTION_A = -0.4178904745
SECTION_B = 0.3792103129

def node_tables():
    root = math.sqrt(7.0)
    outer = math.sqrt(1.0 / 3.0 + 2.0 * root / 21.0)
    inner = math.sqrt(1.0 / 3.0 - 2.0 * root / 21.0)
    points = np.array([-1.0, -outer, -inner, inner, outer, 1.0])
    weights = np.array([1.0 / 15.0, (14.0 - root) / 30.0, (14.0 + root) / 30.0, (14.0 + root) / 30.0, (14.0 - root) / 30.0, 1.0 / 15.0])
    barycen = np.array([1.0 / np.prod([points[source] - points[target] for target in range(6) if target != source]) for source in range(6)])
    matrix = np.zeros((6, 6))
    for source in range(6):
        for target in range(6):
            if target != source:
                matrix[source, target] = barycen[target] / barycen[source] / (points[source] - points[target])
        matrix[source, source] = -np.sum(matrix[source])
    return (matrix, weights)

def contract(field, table):
    flat = field.reshape((-1, field.shape[-1]))
    result = jnp.dot(flat, table, precision=lax.Precision.HIGHEST, preferred_element_type=jnp.float32)
    return result.reshape(field.shape[:-1] + (table.shape[1],))

def deriv_table(matrix, direction):
    eye_six = np.eye(6)
    if direction == 0:
        full = np.kron(matrix, np.eye(36))
    elif direction == 1:
        full = np.kron(eye_six, np.kron(matrix, eye_six))
    else:
        full = np.kron(np.eye(36), matrix)
    return jnp.asarray(full.T, jnp.float32)

def face_table(direction, side):
    nodes = np.arange(216)
    position = [nodes // 36, nodes // 6 % 6, nodes % 6][direction]
    chosen = nodes[position == side]
    table = np.zeros((216, 36))
    table[chosen, np.arange(36)] = 1.0
    return table

def apply_deriv(field, direction, matrix):
    return contract(field, deriv_table(matrix, direction))

def primitives(state):
    density = state[:, :, 0]
    velocity = state[:, :, 1:4] / density[:, :, None]
    pressure = (GAMMA - 1.0) * (state[:, :, 4] - 0.5 * lax.optimization_barrier(jnp.sum(state[:, :, 1:4] * velocity, axis=2)))
    return (density, velocity, pressure)

def phys_flux(state, direction):
    density, velocity, pressure = primitives(state)
    normal_vector = velocity[:, :, direction]
    unit = jnp.asarray(np.eye(3)[direction], jnp.float32).reshape(1, 1, 3, 1, 1)
    momentum = state[:, :, 1:4] * normal_vector[:, :, None] + pressure[:, :, None] * unit
    energy = (state[:, :, 4] + pressure) * normal_vector
    return jnp.concatenate([state[:, :, direction + 1:direction + 2], momentum, energy[:, :, None]], axis=2)

def rusanov(lower, upper, direction):
    rho_lo, vel_lo, pres_lo = primitives(lower)
    rho_hi, vel_hi, pres_hi = primitives(upper)
    speed = jnp.maximum(jnp.abs(vel_lo[:, :, direction]) + jnp.sqrt(GAMMA * pres_lo / rho_lo), jnp.abs(vel_hi[:, :, direction]) + jnp.sqrt(GAMMA * pres_hi / rho_hi))
    return 0.5 * (phys_flux(lower, direction) + phys_flux(upper, direction)) - 0.5 * speed[:, :, None] * (upper - lower)

def mirror(state):
    return jnp.concatenate([state[:, :, 0:1], -state[:, :, 1:4], state[:, :, 4:5]], axis=2)

def split_volume(state, direction, matrix):
    density, velocity, pressure = primitives(state)
    specific = state[:, :, 4] / density
    normal = velocity[:, :, direction]
    others = [velocity[:, :, 0], velocity[:, :, 1], velocity[:, :, 2], specific]
    fields = [density, normal, pressure, density * normal, pressure * normal]
    for other in others:
        fields = fields + [other, normal * other, density * other, density * normal * other]
    derived = apply_deriv(jnp.stack(fields, axis=0), direction, matrix)
    d_rho, d_norm, d_pres, d_mass, d_work = (derived[0], derived[1], derived[2], derived[3], derived[4])

    def triple(member):
        base = 5 + 4 * member
        other = others[member]
        return 0.25 * (derived[base + 3] + density * derived[base + 1] + normal * derived[base + 2] + other * d_mass + density * normal * derived[base] + density * other * d_norm + normal * other * d_rho)
    parts = [0.5 * (density * d_norm + normal * d_rho + d_mass)]
    for member in range(3):
        value = triple(member)
        if member == direction:
            value = value + d_pres
        parts.append(value)
    parts.append(triple(3) + 0.5 * (pressure * d_norm + normal * d_pres + d_work))
    return jnp.stack(parts, axis=2)

def face(field, direction, side):
    return contract(field, jnp.asarray(face_table(direction, side), jnp.float32))

def embed(lower, upper, direction):
    low_table = jnp.asarray(face_table(direction, 0).T, jnp.float32)
    high_table = jnp.asarray(face_table(direction, 5).T, jnp.float32)
    return contract(lower, low_table) + contract(upper, high_table)

def lateral(xfield, zfield):
    return jnp.concatenate([face(xfield, 0, 0), face(xfield, 0, 5), face(zfield, 2, 0), face(zfield, 2, 5)], axis=-1)

def rolled(packed):
    return (jnp.roll(packed, 1, axis=0)[..., 36:72], jnp.roll(packed, -1, axis=0)[..., 0:36], jnp.roll(packed, 1, axis=1)[..., 108:144], jnp.roll(packed, -1, axis=1)[..., 72:108])

def walls(flags):
    solid = flags == 1
    edge = jnp.ones(flags.shape[:2] + (1,), dtype=bool)
    wall_low = jnp.concatenate([edge, solid], axis=2)
    wall_high = jnp.concatenate([solid, edge], axis=2)
    return (wall_low[:, :, None, :, None], wall_high[:, :, None, :, None])

def y_neighbours(bottom, top):
    below = jnp.concatenate([bottom[:, :, :, :1], top[:, :, :, :-1]], axis=3)
    above = jnp.concatenate([bottom[:, :, :, 1:], top[:, :, :, -1:]], axis=3)
    return (below, above)

def to_prim(trace):
    density, velocity, pressure = primitives(trace)
    return jnp.concatenate([velocity, (pressure / density)[:, :, None]], axis=2)

def lift(state, flags, heights, neighbours, matrix, weights):
    prim = to_prim(state)
    wall_low, wall_high = walls(flags)
    flip = jnp.asarray([-1.0, -1.0, -1.0, 1.0], jnp.float32).reshape(1, 1, 4, 1, 1)
    grads = []
    for direction in range(3):
        own_lo = face(prim, direction, 0)
        own_hi = face(prim, direction, 5)
        if direction == 0:
            out_lo, out_hi, scale = (to_prim(neighbours[0]), to_prim(neighbours[1]), 2.0 / LENGTH_X)
        elif direction == 2:
            out_lo, out_hi, scale = (to_prim(neighbours[2]), to_prim(neighbours[3]), 2.0 / LENGTH_Z)
        else:
            below, above = y_neighbours(own_lo, own_hi)
            out_lo = jnp.where(wall_low, own_lo * flip, below)
            out_hi = jnp.where(wall_high, own_hi * flip, above)
            scale = (2.0 / heights).reshape(1, 1, 1, -1, 1)
        surface = embed(-0.5 * (out_lo - own_lo) / weights[0], 0.5 * (out_hi - own_hi) / weights[5], direction)
        grads.append(scale * (apply_deriv(prim, direction, matrix) + surface))
    return (prim, grads)

def viscous(prim, grads):
    spread = grads[0][:, :, 0] + grads[1][:, :, 1] + grads[2][:, :, 2]
    fluxes = []
    for direction in range(3):
        stress = []
        for member in range(3):
            value = VISCOSITY * (grads[direction][:, :, member] + grads[member][:, :, direction])
            if member == direction:
                value = value - 2.0 / 3.0 * VISCOSITY * spread
            stress.append(value)
        energy = prim[:, :, 0] * stress[0] + prim[:, :, 1] * stress[1] + prim[:, :, 2] * stress[2]
        energy = energy + CONDUCT * grads[direction][:, :, 3]
        fluxes.append(jnp.stack(stress + [energy], axis=2))
    return fluxes

def tendency(state, flags, heights, neighbours, fluxes, visc_nbrs, matrix, weights):
    wall_low, wall_high = walls(flags)
    total = jnp.zeros_like(state)
    for direction in range(3):
        own_lo = face(state, direction, 0)
        own_hi = face(state, direction, 5)
        visc_lo = face(fluxes[direction], direction, 0)
        visc_hi = face(fluxes[direction], direction, 5)
        if direction == 1:
            below, above = y_neighbours(own_lo, own_hi)
            star_lo = rusanov(jnp.where(wall_low, mirror(own_lo), below), own_lo, 1)
            star_hi = rusanov(own_hi, jnp.where(wall_high, mirror(own_hi), above), 1)
            vbelow, vabove = y_neighbours(visc_lo, visc_hi)
            vstar_lo = jnp.where(wall_low, visc_lo, 0.5 * (vbelow + visc_lo))
            vstar_hi = jnp.where(wall_high, visc_hi, 0.5 * (vabove + visc_hi))
            scale = (2.0 / heights).reshape(1, 1, 1, -1, 1)
        else:
            slot = 0 if direction == 0 else 2
            star_lo = rusanov(neighbours[slot], own_lo, direction)
            star_hi = rusanov(own_hi, neighbours[slot + 1], direction)
            vstar_lo = 0.5 * (visc_nbrs[slot] + visc_lo)
            vstar_hi = 0.5 * (visc_nbrs[slot + 1] + visc_hi)
            scale = 2.0 / LENGTH_X if direction == 0 else 2.0 / LENGTH_Z
        inv_surface = embed(-(star_lo - phys_flux(own_lo, direction)) / weights[0], (star_hi - phys_flux(own_hi, direction)) / weights[5], direction)
        visc_surface = embed(-(vstar_lo - visc_lo) / weights[0], (vstar_hi - visc_hi) / weights[5], direction)
        visc_all = apply_deriv(fluxes[direction], direction, matrix) + visc_surface
        visc_all = jnp.concatenate([jnp.zeros_like(visc_all[:, :, :1]), visc_all], axis=2)
        total = total + scale * (visc_all - split_volume(state, direction, matrix) - inv_surface)
    return total

def reference(state, register, heights, solid_wall_mask):
    matrix, weights = node_tables()
    neighbours = rolled(lateral(state, state))
    columns = state.shape[0]
    slabs = columns // EX

    def split(array):
        return array.reshape((slabs, EX) + array.shape[1:])

    def first_pass(items):
        block, flags = (items[0], items[1])
        prim, grads = lift(block, flags, heights, items[2:], matrix, weights)
        fluxes = viscous(prim, grads)
        return lateral(fluxes[0], fluxes[2])
    packed = lax.map(first_pass, (split(state), split(solid_wall_mask)) + tuple((split(item) for item in neighbours)))
    packed = packed.reshape((columns,) + packed.shape[2:])
    visc_nbrs = rolled(packed)

    def second_pass(items):
        block, reg, flags = (items[0], items[1], items[2])
        nbrs = items[3:7]
        vnbrs = items[7:11]
        prim, grads = lift(block, flags, heights, nbrs, matrix, weights)
        fluxes = viscous(prim, grads)
        rhs = tendency(block, flags, heights, nbrs, fluxes, vnbrs, matrix, weights)
        reg_next = SECTION_A * reg + TIME_STEP * rhs
        return (block + SECTION_B * reg_next, reg_next)
    inputs = (split(state), split(register), split(solid_wall_mask)) + tuple((split(item) for item in neighbours))
    inputs = inputs + tuple((split(item) for item in visc_nbrs))
    state_next, register_next = lax.map(second_pass, inputs)
    return (state_next.reshape(state.shape), register_next.reshape(state.shape))
```

```python
import functools
import math

import jax
import jax.numpy as jnp
import numpy as np
from jax import lax
from jax.experimental import pallas as pl
from jax.experimental.pallas import tpu as pltpu
from jax.sharding import PartitionSpec as P

GAMMA = 1.4
VISCOSITY = 0.001
CONDUCT = 0.001 * 1.4 / (0.4 * 0.72)
SCALE_X = 2.0 / 0.2
SCALE_Z = 2.0 / 0.15
TIME_STEP = 0.004
SECTION_A = -0.4178904745
SECTION_B = 0.3792103129
HALF_W = 7.5

ROWS, NODES = (48, 216)
F32, BF16 = (jnp.float32, jnp.bfloat16)


def node_matrix():
    root = math.sqrt(7.0)
    outer = math.sqrt(1.0 / 3.0 + 2.0 * root / 21.0)
    inner = math.sqrt(1.0 / 3.0 - 2.0 * root / 21.0)
    points = np.array([-1.0, -outer, -inner, inner, outer, 1.0])
    barycen = np.array(
        [1.0 / np.prod([points[i] - points[j] for j in range(6) if j != i]) for i in range(6)]
    )
    matrix = np.zeros((6, 6))
    for i in range(6):
        for j in range(6):
            if j != i:
                matrix[i, j] = barycen[j] / barycen[i] / (points[i] - points[j])
        matrix[i, i] = -np.sum(matrix[i])
    return matrix


STRIDE = (36, 6, 1)


def coefficients():
    matrix = node_matrix()
    nodes = np.arange(NODES)
    place = (nodes // 36, nodes // 6 % 6, nodes % 6)
    rows = [matrix[place[d], j] for d in range(3) for j in range(6)]
    return np.stack(rows).astype(np.float32)


def tables():
    nodes = np.arange(NODES)
    low_face = nodes[nodes % 6 == 0]
    unpack = np.zeros((2, 3, 128, NODES), np.float32)
    corner_unpack = np.zeros((2, 3, 128, NODES), np.float32)
    for j in range(3):
        slot = 36 * j + np.arange(36)
        unpack[0, j, slot, low_face] = 1.0
        unpack[1, j, slot, low_face + 5] = 1.0
        for iy in range(6):
            slot = 108 + 6 * j + iy
            for ix in (0, 5):
                base = 36 * ix + 6 * iy
                corner_unpack[0, j, slot, base] = 1.0
                corner_unpack[1, j, slot, base + 5] = 1.0
    return dict(uz=unpack.astype(jnp.bfloat16), cu=corner_unpack.astype(jnp.bfloat16))


def one_hot(source, depth):
    rows = lax.broadcasted_iota(jnp.int32, (depth, source.shape[1]), 0)
    return jnp.where(rows == source, 1.0, 0.0).astype(BF16)


def x_pack_table(side, j):
    lane = lax.broadcasted_iota(jnp.int32, (1, 128), 1) - 36 * j
    inside = jnp.logical_and(lane >= 0, lane < 36)
    return one_hot(jnp.where(inside, lane + (180 if side == 0 else 0), -1), NODES)


def x_unpack_table(side, j):
    lane = lax.broadcasted_iota(jnp.int32, (1, NODES), 1) - (0 if side == 0 else 180)
    inside = jnp.logical_and(lane >= 0, lane < 36)
    return one_hot(jnp.where(inside, lane + 36 * j, -1), 128)


def z_pack_table(side, j):
    lane = lax.broadcasted_iota(jnp.int32, (1, 128), 1) - 36 * j
    inside = jnp.logical_and(lane >= 0, lane < 36)
    return one_hot(jnp.where(inside, 6 * lane + (5 if side == 0 else 0), -1), NODES)


def corner_pack_table(side, j):
    lane = lax.broadcasted_iota(jnp.int32, (1, 128), 1) - (108 + 6 * j)
    inside = jnp.logical_and(lane >= 0, lane < 6)
    source = jnp.where(inside, 6 * lane + (5 if side == 0 else 0), -1000)
    return one_hot(source, NODES) + one_hot(source + 180, NODES)


def pick_table(side):
    row = lax.broadcasted_iota(jnp.int32, (24, ROWS), 0)
    column = lax.broadcasted_iota(jnp.int32, (24, ROWS), 1)
    return jnp.where(column == 2 * row + (1 - side), 1.0, 0.0).astype(BF16)


def swap_table(lanes, d):
    lane = lax.broadcasted_iota(jnp.int32, (1, NODES), 1)
    step = 5 * STRIDE[d]
    return one_hot(
        jnp.where(lanes.lo[d], lane + step, jnp.where(lanes.hi[d], lane - step, -1)), NODES
    )


def deriv_table(lanes, coef_ref, d):
    lane = lax.broadcasted_iota(jnp.int32, (1, NODES), 1)
    base = lane - STRIDE[d] * lanes.place[d]
    rows = lax.broadcasted_iota(jnp.int32, (NODES, NODES), 0) - base
    table = jnp.zeros((NODES, NODES), F32)
    for j in range(6):
        line = coef_ref[6 * d + j : 6 * d + j + 1, :]
        table = jnp.where(rows == STRIDE[d] * j, line, table)
    return table


def halves(value):
    high = value.astype(BF16)
    return (high, (value - high.astype(F32)).astype(BF16))


def dot(a, b):
    return jnp.dot(a, b, preferred_element_type=F32)


def derive(pair, dh, dl):
    return dot(pair[0], dh) + (dot(pair[1], dh) + dot(pair[0], dl))


def move(pair, table):
    return dot(pair[0], table) + dot(pair[1], table)


def stack(fields):
    return jnp.concatenate(fields, axis=0)


def rows_of(value, count, size=ROWS):
    return [value[i * size : (i + 1) * size] for i in range(count)]


class Lanes:
    def __init__(self):
        lane = lax.broadcasted_iota(jnp.int32, (1, NODES), 1)
        row = lax.broadcasted_iota(jnp.int32, (ROWS, 1), 0)
        self.a, self.c = (row // 24, row % 2)
        self.k = (row % 24) // 2
        place = (lane // 36, lane // 6 % 6, lane % 6)
        self.place = place
        self.lo = [p == 0 for p in place]
        self.hi = [p == 5 for p in place]
        self.sig = [
            jnp.where(p == 0, 1.0, 0.0) + jnp.where(p == 5, -1.0, 0.0) for p in place
        ]
        self.face = [jnp.logical_or(lo, hi) for lo, hi in zip(self.lo, self.hi)]
        self.ghost_x = jnp.logical_or(
            jnp.logical_and(self.a == 0, self.lo[0]), jnp.logical_and(self.a == 1, self.hi[0])
        )
        self.ghost_z = jnp.logical_or(
            jnp.logical_and(self.c == 0, self.lo[2]), jnp.logical_and(self.c == 1, self.hi[2])
        )


def read_rows(ref, field):
    return stack([ref[a, field].reshape(24, NODES) for a in range(2)])


def write_rows(ref, field, value):
    for a in range(2):
        ref[a, field] = value[24 * a : 24 * a + 24].reshape(12, 2, NODES)


def load_prims(state_ref):
    rho = state_ref[0]
    inv = 1.0 / rho
    mom = [state_ref[1], state_ref[2], state_ref[3]]
    vel = [m * inv for m in mom]
    energy = state_ref[4]
    pres = (GAMMA - 1.0) * (
        energy - 0.5 * (mom[0] * vel[0] + mom[1] * vel[1] + mom[2] * vel[2])
    )
    return (rho, mom, energy, vel, pres, pres * inv, inv)


def walls_of(mask_ref, lanes):
    spread = jnp.zeros((ROWS, 11), jnp.int32)
    for a in range(2):
        for c in range(2):
            here = jnp.logical_and(lanes.a == a, lanes.c == c)
            spread = jnp.where(here, mask_ref[a, c : c + 1, :], spread)
    column = lax.broadcasted_iota(jnp.int32, (ROWS, 11), 1)
    solid = jnp.where(spread == 1, 1.0, 0.0)
    low = jnp.sum(jnp.where(column == lanes.k - 1, solid, 0.0), axis=1, keepdims=True)
    high = jnp.sum(jnp.where(column == lanes.k, solid, 0.0), axis=1, keepdims=True)
    return (
        jnp.logical_or(low > 0.5, lanes.k == 0),
        jnp.logical_or(high > 0.5, lanes.k == 11),
    )


def scale_y(h_ref, lanes):
    column = lax.broadcasted_iota(jnp.int32, (ROWS, 12), 1)
    own = jnp.where(column == lanes.k, h_ref[0:1, :], 0.0)
    return 2.0 / jnp.sum(own, axis=1, keepdims=True)


def shift(value, by):
    return pltpu.roll(value, by % value.shape[0], 0)


def inner_x(swapped, own, lanes):
    other = stack([swapped[24:48], swapped[0:24]])
    return jnp.where(jnp.logical_and(lanes.face[0], jnp.logical_not(lanes.ghost_x)), other, own)


def inner_z(swapped, own, lanes):
    other = jnp.where(lanes.lo[2], shift(swapped, 1), shift(swapped, -1))
    return jnp.where(jnp.logical_and(lanes.face[2], jnp.logical_not(lanes.ghost_z)), other, own)


def inner_y(swapped, own, lanes, wall_lo, wall_hi, sign):
    other = jnp.where(lanes.lo[1], shift(swapped, 2), shift(swapped, -2))
    solid = jnp.logical_or(
        jnp.logical_and(wall_lo, lanes.lo[1]), jnp.logical_and(wall_hi, lanes.hi[1])
    )
    return jnp.where(lanes.face[1], jnp.where(solid, sign * own, other), own)


def stress(grads):
    gx, gy, gz = grads
    third = (2.0 / 3.0) * VISCOSITY * (gx[0] + gy[1] + gz[2])
    return [
        2.0 * VISCOSITY * gx[0] - third,
        2.0 * VISCOSITY * gy[1] - third,
        2.0 * VISCOSITY * gz[2] - third,
        VISCOSITY * (gx[1] + gy[0]),
        VISCOSITY * (gx[2] + gz[0]),
        VISCOSITY * (gy[2] + gz[1]),
        CONDUCT * gx[3],
        CONDUCT * gy[3],
        CONDUCT * gz[3],
    ]


def add_lift(tg, delta, direction):
    tg = list(tg)
    bulk = (2.0 / 3.0) * VISCOSITY * delta[direction]
    for d in range(3):
        tg[d] = tg[d] - bulk
    tg[direction] = tg[direction] + 2.0 * VISCOSITY * delta[direction]
    for other in range(3):
        if other != direction:
            slot = {1: 3, 2: 4, 3: 5}[direction + other]
            tg[slot] = tg[slot] + VISCOSITY * delta[other]
    tg[6 + direction] = tg[6 + direction] + CONDUCT * delta[3]
    return tg


def flux_of(tg, vel, direction):
    t = [
        (tg[0], tg[3], tg[4]),
        (tg[3], tg[1], tg[5]),
        (tg[4], tg[5], tg[2]),
    ][direction]
    work = vel[0] * t[0] + vel[1] * t[1] + vel[2] * t[2] + tg[6 + direction]
    return [t[0], t[1], t[2], work]


def ghost_lift(flux, vel, delta, direction, lift_direction):
    zero = jnp.zeros_like(delta[0])
    tg = add_lift([zero] * 9, delta, lift_direction)
    change = flux_of(tg, vel, direction)
    return [f + d for f, d in zip(flux, change)]


def pack_faces(fields, table_of, side):
    total = None
    for j in range(3):
        part = halves(stack([fields[3 * s + j] for s in range(3)]))
        value = move(part, table_of(side, j))
        total = value if total is None else total + value
    return total


def euler(rho, vel, pres, direction):
    normal = vel[direction]
    mass = rho * normal
    square = vel[0] * vel[0] + vel[1] * vel[1] + vel[2] * vel[2]
    energy = pres * (1.0 / (GAMMA - 1.0)) + 0.5 * rho * square
    flux = [mass] + [mass * v for v in vel] + [(energy + pres) * normal]
    flux[1 + direction] = flux[1 + direction] + pres
    state = [rho, rho * vel[0], rho * vel[1], rho * vel[2], energy]
    return (flux, state)


def face_terms(own, out, direction, sig, scale):
    rho, vel, temp = own
    rho_out, vel_out, temp_out = out
    flux, state = euler(rho, vel, rho * temp, direction)
    flux_out, state_out = euler(rho_out, vel_out, rho_out * temp_out, direction)
    speed = jnp.maximum(
        jnp.abs(vel[direction]) + jnp.sqrt(GAMMA * temp),
        jnp.abs(vel_out[direction]) + jnp.sqrt(GAMMA * temp_out),
    )
    speed = speed * jnp.abs(sig)
    return [
        (HALF_W * scale) * (sig * (fo - fi) + speed * (so - si))
        for fi, fo, si, so in zip(flux, flux_out, state, state_out)
    ]


def parity_of(axis):
    return lax.rem(lax.axis_index(axis), 2) == 0


def first_kernel(state_hbm, mask_hbm, h_hbm, coef_hbm, st_ref, aux_ref, dh_ref, dl_ref, sw_ref, tg_ref,
                 even_ref, odd_ref, state_buf, mask_buf, h_buf, coef_buf, sems):
    copies = [
        pltpu.make_async_copy(src, dst, sems.at[i])
        for i, (src, dst) in enumerate(
            ((coef_hbm, coef_buf), (state_hbm, state_buf), (mask_hbm, mask_buf), (h_hbm, h_buf))
        )
    ]
    for copy in copies:
        copy.start()
    lanes = Lanes()
    for d in range(3):
        sw_ref[d] = swap_table(lanes, d)
    copies[0].wait()
    for d in range(3):
        high, low = halves(deriv_table(lanes, coef_buf, d))
        dh_ref[d] = high
        dl_ref[d] = low
    for copy in copies[1:]:
        copy.wait()
    for i in range(5):
        st_ref[i] = read_rows(state_buf, i)
    rho, _, _, vel, _, temp, _ = load_prims(st_ref)
    wall_lo, wall_hi = walls_of(mask_buf, lanes)
    sy = scale_y(h_buf, lanes)
    slot = lax.broadcasted_iota(jnp.int32, (ROWS, 128), 1)
    aux_ref[...] = jnp.where(
        slot == 0,
        jnp.where(wall_lo, 1.0, 0.0),
        jnp.where(slot == 1, jnp.where(wall_hi, 1.0, 0.0), sy),
    )
    own = vel + [temp]
    pair = halves(stack(own))
    scales = (SCALE_X, sy, SCALE_Z)
    grads = []
    for d in range(3):
        slope = rows_of(derive(pair, dh_ref[d], dl_ref[d]), 4)
        swapped = rows_of(move(pair, sw_ref[d]), 4)
        grad = []
        for i in range(4):
            if d == 0:
                out = inner_x(swapped[i], own[i], lanes)
            elif d == 2:
                out = inner_z(swapped[i], own[i], lanes)
            else:
                sign = 1.0 if i == 3 else -1.0
                out = inner_y(swapped[i], own[i], lanes, wall_lo, wall_hi, sign)
            grad.append(scales[d] * (slope[i] + (HALF_W * lanes.sig[d]) * (own[i] - out)))
        grads.append(grad)
    tg = stress(grads)
    for i in range(9):
        tg_ref[i] = tg[i]
    fields = [rho] + own + flux_of(tg, vel, 0)
    up = pack_faces([f[24:48] for f in fields], x_pack_table, 0)
    down = pack_faces([f[0:24] for f in fields], x_pack_table, 1)
    even = parity_of("gx")
    even_ref[...] = jnp.where(even, up, down)
    odd_ref[...] = jnp.where(even, down, up)


def aux_of(aux_ref):
    return (aux_ref[:, 0:1] > 0.5, aux_ref[:, 1:2] > 0.5, aux_ref[:, 2:3])


def volume_kernel(state_ref, aux_ref, dh_ref, dl_ref, sw_ref, out_ref, ux_ref, pz_ref, cp_ref):
    lanes = Lanes()
    rho, mom, energy, vel, pres, temp, inv = load_prims(state_ref)
    wall_lo, wall_hi, sy = aux_of(aux_ref)
    scales = (SCALE_X, sy, SCALE_Z)
    spec = energy * inv
    common = halves(stack([rho] + vel + [pres, spec] + mom + [energy]))
    swap_pair = halves(stack([rho] + vel + [temp]))
    others = vel + [spec]
    dens = mom + [energy]
    own = [rho] + vel + [temp]
    total = [None] * 5
    for d in range(3):
        normal = vel[d]
        mine = [pres * normal] + [normal * o for o in others] + [normal * m for m in dens]
        base = rows_of(derive(common, dh_ref[d], dl_ref[d]), 10)
        rest = rows_of(derive(halves(stack(mine)), dh_ref[d], dl_ref[d]), 9)
        d_rho, d_pres, d_work = (base[0], base[4], rest[0])
        d_others = base[1:4] + [base[5]]
        d_dens = base[6:10]
        d_norm, d_mass = (base[1 + d], base[6 + d])
        mass = mom[d]
        parts = [0.5 * (rho * d_norm + normal * d_rho + d_mass)]
        for m in range(4):
            value = 0.25 * (
                rest[5 + m]
                + rho * rest[1 + m]
                + normal * d_dens[m]
                + others[m] * (d_mass + rho * d_norm + normal * d_rho)
                + mass * d_others[m]
            )
            if m == d:
                value = value + d_pres
            if m == 3:
                value = value + 0.5 * (pres * d_norm + normal * d_pres + d_work)
            parts.append(value)
        swapped = rows_of(move(swap_pair, sw_ref[d]), 5)
        outs = []
        for i in range(5):
            if d == 0:
                outs.append(inner_x(swapped[i], own[i], lanes))
            elif d == 2:
                outs.append(inner_z(swapped[i], own[i], lanes))
            else:
                sign = -1.0 if i in (1, 2, 3) else 1.0
                outs.append(inner_y(swapped[i], own[i], lanes, wall_lo, wall_hi, sign))
        faces = face_terms(
            (rho, vel, temp), (outs[0], outs[1:4], outs[4]), d, lanes.sig[d], scales[d]
        )
        for i in range(5):
            value = faces[i] - scales[d] * parts[i]
            total[i] = value if d == 0 else total[i] + value
    for i in range(5):
        out_ref[i] = total[i]
    for side in range(2):
        for j in range(3):
            ux_ref[side, j] = x_unpack_table(side, j)
            pz_ref[side, j] = z_pack_table(side, j)
            cp_ref[side, j] = corner_pack_table(side, j)


def sides_of(even_ref, odd_ref, axis):
    even = parity_of(axis)
    return (
        jnp.where(even, odd_ref[...], even_ref[...]),
        jnp.where(even, even_ref[...], odd_ref[...]),
    )


def unpack_faces(lower, upper, table_ref, spread):
    first, second = (halves(lower), halves(upper))
    fields = [None] * 9
    for j in range(3):
        low = rows_of(move(first, table_ref[0, j]), 3, 24)
        high = rows_of(move(second, table_ref[1, j]), 3, 24)
        for s in range(3):
            fields[3 * s + j] = spread(low[s], high[s])
    return fields


def second_kernel(state_ref, tg_ref, even_ref, odd_ref, ux_ref, pz_ref, cp_ref,
                  tgo_ref, gx_ref, even_out, odd_out):
    lanes = Lanes()
    rho, _, _, vel, _, temp, _ = load_prims(state_ref)
    own = vel + [temp]
    lower, upper = sides_of(even_ref, odd_ref, "gx")
    ghost = unpack_faces(lower, upper, ux_ref, lambda lo, hi: stack([lo, hi]))
    weight = (SCALE_X * HALF_W) * lanes.sig[0] * jnp.where(lanes.ghost_x, 1.0, 0.0)
    delta = [weight * (o - g) for o, g in zip(own, ghost[1:5])]
    tg = add_lift([tg_ref[i] for i in range(9)], delta, 0)
    for i in range(9):
        tgo_ref[i] = tg[i]
    flux = ghost_lift(ghost[5:9], ghost[1:4], delta, 0, 0)
    for i, field in enumerate(ghost[:5] + flux):
        gx_ref[i] = field
    fields = [rho] + own + flux_of(tg, vel, 2)
    corner = [jnp.where(lanes.ghost_x, g, 0.0) for g in ghost[1:5]]
    messages = []
    for side in (0, 1):
        total = None
        for j in range(3):
            picked = [fields[3 * s + j] for s in range(3)]
            part = move(halves(stack(picked)), pz_ref[side, j])
            total = part if total is None else total + part
        edges = move(halves(stack([corner[0], corner[3]])), cp_ref[side, 0])
        first = edges[0:48]
        for j in (1, 2):
            first = first + move(halves(corner[j]), cp_ref[side, j])
        total = total + stack([first, edges[48:96], jnp.zeros((ROWS, 128), F32)])
        pick = pick_table(side)
        kept = []
        for s in range(3):
            high, low = halves(total[48 * s : 48 * s + 48])
            kept.append(dot(pick, high) + dot(pick, low))
        messages.append(stack(kept))
    even = parity_of("gz")
    even_out[...] = jnp.where(even, messages[0], messages[1])
    odd_out[...] = jnp.where(even, messages[1], messages[0])


def last_kernel(state_ref, reg_ref, vol_ref, tg_ref, gx_ref, aux_ref, even_ref, odd_ref,
                dh_ref, dl_ref, sw_ref, uz_ref, cu_ref, ri_ref, state_out, reg_out):
    lanes = Lanes()
    rho, mom, energy, vel, _, temp, _ = load_prims(state_ref)
    wall_lo, wall_hi, sy = aux_of(aux_ref)
    scales = (SCALE_X, sy, SCALE_Z)
    own = vel + [temp]
    lower, upper = sides_of(even_ref, odd_ref, "gz")

    def widen(value, side):
        put = ri_ref[side]
        parts = []
        for s in range(3):
            high, low = halves(value[24 * s : 24 * s + 24, :])
            parts.append(dot(put, high) + dot(put, low))
        return stack(parts)

    first, second = (halves(widen(lower, 0)), halves(widen(upper, 1)))
    ghost_z = [None] * 9
    corner = [None] * 4
    for j in range(3):
        value = rows_of(move(first, uz_ref[0, j]) + move(second, uz_ref[1, j]), 3)
        edge = rows_of(move(first, cu_ref[0, j]) + move(second, cu_ref[1, j]), 3)
        for s in range(3):
            ghost_z[3 * s + j] = value[s]
        corner[j] = edge[0]
        if j == 0:
            corner[3] = edge[1]
    keep_x = jnp.where(lanes.ghost_x, 1.0, 0.0)
    keep_z = jnp.where(lanes.ghost_z, 1.0, 0.0)
    ghost_x = [gx_ref[i] for i in range(9)]
    weight = (SCALE_Z * HALF_W) * lanes.sig[2] * keep_z
    delta = [weight * (o - g) for o, g in zip(own, ghost_z[1:5])]
    tg = add_lift([tg_ref[i] for i in range(9)], delta, 2)
    flux_z = ghost_lift(ghost_z[5:9], ghost_z[1:4], delta, 2, 2)
    edge_delta = [(weight * keep_x) * (g - c) for g, c in zip(ghost_x[1:5], corner)]
    flux_x = ghost_lift(ghost_x[5:9], ghost_x[1:4], edge_delta, 0, 2)
    total = [vol_ref[i] for i in range(5)]
    for d, ghost, keep in ((0, ghost_x, lanes.ghost_x), (2, ghost_z, lanes.ghost_z)):
        out = [jnp.where(keep, g, o) for g, o in zip(ghost[:5], [rho] + own)]
        faces = face_terms(
            (rho, vel, temp), (out[0], out[1:4], out[4]), d, lanes.sig[d], scales[d]
        )
        total = [t + f for t, f in zip(total, faces)]
    for d in range(3):
        flux = flux_of(tg, vel, d)
        pair = halves(stack(flux))
        slope = rows_of(derive(pair, dh_ref[d], dl_ref[d]), 4)
        swapped = rows_of(move(pair, sw_ref[d]), 4)
        for i in range(4):
            if d == 0:
                out = jnp.where(lanes.ghost_x, flux_x[i], inner_x(swapped[i], flux[i], lanes))
            elif d == 2:
                out = jnp.where(lanes.ghost_z, flux_z[i], inner_z(swapped[i], flux[i], lanes))
            else:
                out = inner_y(swapped[i], flux[i], lanes, wall_lo, wall_hi, 1.0)
            total[i + 1] = total[i + 1] + scales[d] * (
                slope[i] + (HALF_W * lanes.sig[d]) * (flux[i] - out)
            )
    for i, field in enumerate([rho] + mom + [energy]):
        reg = SECTION_A * read_rows(reg_ref, i) + TIME_STEP * total[i]
        write_rows(reg_out, i, reg)
        write_rows(state_out, i, field + SECTION_B * reg)


def row_table():
    put = np.zeros((2, ROWS, 24), np.float32)
    for i in range(24):
        put[0, 2 * i, i] = 1.0
        put[1, 2 * i + 1, i] = 1.0
    return put.astype(jnp.bfloat16)


def field_shape(count):
    return jax.ShapeDtypeStruct((count, ROWS, NODES), F32)


LIMIT = 20 * 1024 * 1024
FACE = jax.ShapeDtypeStruct((72, 128), F32)


def call(kernel, outs, name, flops, **more):
    return pl.pallas_call(
        kernel,
        out_shape=outs,
        name=name,
        compiler_params=pltpu.CompilerParams(vmem_limit_bytes=LIMIT),
        cost_estimate=pl.CostEstimate(flops=flops, bytes_accessed=2_000_000, transcendentals=0),
        **more,
    )


def swap_pairs(axis):
    size = lax.axis_size(axis)
    even = [(i, i ^ 1) for i in range(size)]
    odd = [(i, (i + 1) % size if i % 2 else (i - 1) % size) for i in range(size)]
    return (even, odd)


def shards(state, register, heights, solid_wall_mask):
    t = {key: jnp.asarray(value) for key, value in tables().items()}
    put = jnp.asarray(row_table())
    coef = jnp.asarray(coefficients())
    h = heights.reshape(1, 12)

    def rows(array):
        return jnp.transpose(array, (0, 2, 3, 1, 4))

    def unrows(array):
        return jnp.transpose(array, (0, 3, 1, 2, 4))

    reg = rows(register)
    whole = jax.ShapeDtypeStruct((2, 5, 12, 2, NODES), F32)
    table = jax.ShapeDtypeStruct((3, NODES, NODES), BF16)
    aux_shape = jax.ShapeDtypeStruct((ROWS, 128), F32)
    hbm = pl.BlockSpec(memory_space=pltpu.HBM)
    st, aux, dh, dl, sw, tg, even_x, odd_x = call(
        first_kernel,
        (field_shape(5), aux_shape, table, table, table, field_shape(9), FACE, FACE),
        "first",
        10**8,
        in_specs=[hbm] * 4,
        scratch_shapes=[
            pltpu.VMEM((2, 5, 12, 2, NODES), F32),
            pltpu.VMEM((2, 2, 11), jnp.int32),
            pltpu.VMEM((1, 12), F32),
            pltpu.VMEM((18, NODES), F32),
            pltpu.SemaphoreType.DMA((4,)),
        ],
    )(*[pltpu.with_memory_space_constraint(v, pltpu.HBM) for v in (rows(state), solid_wall_mask, h, coef)])
    even, odd = swap_pairs("gx")
    even_x = lax.ppermute(even_x, "gx", even)
    odd_x = lax.ppermute(odd_x, "gx", odd)
    pack = jax.ShapeDtypeStruct((2, 3, NODES, 128), BF16)
    unpack = jax.ShapeDtypeStruct((2, 3, 128, NODES), BF16)
    vol, ux, pz, cp = call(
        volume_kernel, (field_shape(5), unpack, pack, pack), "volume", 10**9
    )(st, aux, dh, dl, sw)
    tg, gx, even_z, odd_z = call(
        second_kernel, (field_shape(9), field_shape(9), FACE, FACE), "second", 10**8
    )(st, tg, even_x, odd_x, ux, pz, cp)
    even, odd = swap_pairs("gz")
    even_z = lax.ppermute(even_z, "gz", even)
    odd_z = lax.ppermute(odd_z, "gz", odd)
    state_next, reg_next = call(last_kernel, (whole, whole), "last", 10**8)(
        st, reg, vol, tg, gx, aux, even_z, odd_z, dh, dl, sw, t["uz"], t["cu"], put,
    )
    return (unrows(state_next), unrows(reg_next))


def solution(mesh):
    spec = P("gx", "gz", None, None, None)
    return jax.shard_map(
        shards,
        mesh=mesh,
        in_specs=(spec, spec, P(), P("gx", "gz", None)),
        out_specs=(spec, spec),
        check_vma=False,
    )
```

```python
import math

import jax
import jax.numpy as jnp
import numpy as np
from jax import lax
from jax.experimental import pallas as pl
from jax.experimental.pallas import tpu as pltpu
from jax.sharding import PartitionSpec as P


GAMMA = 1.4
VISCOSITY = 0.001
CONDUCT = 0.001 * 1.4 / (0.4 * 0.72)
SCALE_X = 2.0 / 0.2
SCALE_Z = 2.0 / 0.15
TIME_STEP = 0.004
SECTION_A = -0.4178904745
SECTION_B = 0.3792103129
HALF_W = 7.5


ROWS, NODES = (48, 216)
F32, BF16 = (jnp.float32, jnp.bfloat16)


def node_matrix():
    root = math.sqrt(7.0)
    outer = math.sqrt(1.0 / 3.0 + 2.0 * root / 21.0)
    inner = math.sqrt(1.0 / 3.0 - 2.0 * root / 21.0)
    points = np.array([-1.0, -outer, -inner, inner, outer, 1.0])
    barycen = np.array(
        [1.0 / np.prod([points[i] - points[j] for j in range(6) if j != i]) for i in range(6)]
    )
    matrix = np.zeros((6, 6))
    for i in range(6):
        for j in range(6):
            if j != i:
                matrix[i, j] = barycen[j] / barycen[i] / (points[i] - points[j])
        matrix[i, i] = -np.sum(matrix[i])
    return matrix


STRIDE = (36, 6, 1)


def coefficients():
    matrix = node_matrix()
    nodes = np.arange(NODES)
    place = (nodes // 36, nodes // 6 % 6, nodes % 6)
    rows = [matrix[place[d], j] for d in range(3) for j in range(6)]
    return np.stack(rows).astype(np.float32)


def hot(sources, depth):
    rows = lax.broadcasted_iota(jnp.int32, (depth, sources[0].shape[1]), 0)
    found = rows == sources[0]
    for source in sources[1:]:
        found = jnp.logical_or(found, rows == source)
    return jnp.where(found, 1.0, 0.0).astype(BF16)


def slot_lane(first, width):
    lane = lax.broadcasted_iota(jnp.int32, (1, 128), 1) - first
    return jnp.where(jnp.logical_and(lane >= 0, lane < width), lane, -1000)


def pack_table(d, j):
    node = slot_lane(36 * j, 36) * (1 if d == 0 else 6)
    return hot([node, node + 5 * STRIDE[d]], NODES)


def unpack_table(lanes, d, j):
    node = lax.broadcasted_iota(jnp.int32, (1, NODES), 1)
    face = (node % 36) if d == 0 else node // 6
    return hot([jnp.where(lanes.face[d], 36 * j + face, -1)], 128)


def edge_pack_table(j):
    node = 6 * slot_lane(108 + 6 * j, 6)
    return hot([node, node + 5, node + 180, node + 185], NODES)


def edge_unpack_table(lanes, j):
    edge = jnp.logical_and(lanes.face[0], lanes.face[2])
    return hot([jnp.where(edge, 108 + 6 * j + lanes.place[1], -1)], 128)


def swap_table(lanes, d):
    lane = lax.broadcasted_iota(jnp.int32, (1, NODES), 1)
    step = 5 * STRIDE[d]
    return hot(
        [jnp.where(lanes.lo[d], lane + step, jnp.where(lanes.hi[d], lane - step, -1))], NODES
    )


def deriv_table(lanes, coef_ref, d):
    lane = lax.broadcasted_iota(jnp.int32, (1, NODES), 1)
    base = lane - STRIDE[d] * lanes.place[d]
    rows = lax.broadcasted_iota(jnp.int32, (NODES, NODES), 0) - base
    table = jnp.zeros((NODES, NODES), F32)
    for j in range(6):
        line = coef_ref[6 * d + j : 6 * d + j + 1, :]
        table = jnp.where(rows == STRIDE[d] * j, line, table)
    return table


def halves(value):
    high = value.astype(BF16)
    return (high, (value - high.astype(F32)).astype(BF16))


def dot(a, b):
    return jnp.dot(a, b, preferred_element_type=F32)


def derive(pair, dh, dl):
    return dot(pair[0], dh) + (dot(pair[1], dh) + dot(pair[0], dl))


def move(pair, table):
    return dot(pair[0], table) + dot(pair[1], table)


def stack(fields):
    return jnp.concatenate(fields, axis=0)


def rows_of(value, count, size=ROWS):
    return [value[i * size : (i + 1) * size] for i in range(count)]


class Lanes:
    def __init__(self):
        lane = lax.broadcasted_iota(jnp.int32, (1, NODES), 1)
        row = lax.broadcasted_iota(jnp.int32, (ROWS, 1), 0)
        self.a, self.c = (row // 24, row % 2)
        self.k = (row % 24) // 2
        place = (lane // 36, lane // 6 % 6, lane % 6)
        self.place = place
        self.lo = [p == 0 for p in place]
        self.hi = [p == 5 for p in place]
        self.sig = [
            jnp.where(p == 0, 1.0, 0.0) + jnp.where(p == 5, -1.0, 0.0) for p in place
        ]
        self.face = [jnp.logical_or(lo, hi) for lo, hi in zip(self.lo, self.hi)]
        self.ghost_x = jnp.logical_or(
            jnp.logical_and(self.a == 0, self.lo[0]), jnp.logical_and(self.a == 1, self.hi[0])
        )
        self.ghost_z = jnp.logical_or(
            jnp.logical_and(self.c == 0, self.lo[2]), jnp.logical_and(self.c == 1, self.hi[2])
        )


def read_rows(ref, field):
    return stack([ref[a, field].reshape(24, NODES) for a in range(2)])


def write_rows(ref, field, value):
    for a in range(2):
        ref[a, field] = value[24 * a : 24 * a + 24].reshape(12, 2, NODES)


def load_prims(state_ref):
    rho = state_ref[0]
    inv = 1.0 / rho
    mom = [state_ref[1], state_ref[2], state_ref[3]]
    vel = [m * inv for m in mom]
    energy = state_ref[4]
    pres = (GAMMA - 1.0) * (
        energy - 0.5 * (mom[0] * vel[0] + mom[1] * vel[1] + mom[2] * vel[2])
    )
    return (rho, mom, energy, vel, pres, pres * inv, inv)


def walls_of(mask_ref, lanes):
    spread = jnp.zeros((ROWS, 11), jnp.int32)
    for a in range(2):
        for c in range(2):
            here = jnp.logical_and(lanes.a == a, lanes.c == c)
            spread = jnp.where(here, mask_ref[a, c : c + 1, :], spread)
    column = lax.broadcasted_iota(jnp.int32, (ROWS, 11), 1)
    solid = jnp.where(spread == 1, 1.0, 0.0)
    low = jnp.sum(jnp.where(column == lanes.k - 1, solid, 0.0), axis=1, keepdims=True)
    high = jnp.sum(jnp.where(column == lanes.k, solid, 0.0), axis=1, keepdims=True)
    return (
        jnp.logical_or(low > 0.5, lanes.k == 0),
        jnp.logical_or(high > 0.5, lanes.k == 11),
    )


def scale_y(h_ref, lanes):
    column = lax.broadcasted_iota(jnp.int32, (ROWS, 12), 1)
    own = jnp.where(column == lanes.k, h_ref[0:1, :], 0.0)
    return 2.0 / jnp.sum(own, axis=1, keepdims=True)


def shift(value, by):
    return pltpu.roll(value, by % value.shape[0], 0)


def inner_x(swapped, own, lanes):
    other = stack([swapped[24:48], swapped[0:24]])
    return jnp.where(jnp.logical_and(lanes.face[0], jnp.logical_not(lanes.ghost_x)), other, own)


def inner_z(swapped, own, lanes):
    other = jnp.where(lanes.lo[2], shift(swapped, 1), shift(swapped, -1))
    return jnp.where(jnp.logical_and(lanes.face[2], jnp.logical_not(lanes.ghost_z)), other, own)


def inner_y(swapped, own, lanes, wall_lo, wall_hi, sign):
    other = jnp.where(lanes.lo[1], shift(swapped, 2), shift(swapped, -2))
    solid = jnp.logical_or(
        jnp.logical_and(wall_lo, lanes.lo[1]), jnp.logical_and(wall_hi, lanes.hi[1])
    )
    return jnp.where(lanes.face[1], jnp.where(solid, sign * own, other), own)


def stress(grads):
    gx, gy, gz = grads
    third = (2.0 / 3.0) * VISCOSITY * (gx[0] + gy[1] + gz[2])
    return [
        2.0 * VISCOSITY * gx[0] - third,
        2.0 * VISCOSITY * gy[1] - third,
        2.0 * VISCOSITY * gz[2] - third,
        VISCOSITY * (gx[1] + gy[0]),
        VISCOSITY * (gx[2] + gz[0]),
        VISCOSITY * (gy[2] + gz[1]),
        CONDUCT * gx[3],
        CONDUCT * gy[3],
        CONDUCT * gz[3],
    ]


def add_lift(tg, delta, direction):
    tg = list(tg)
    bulk = (2.0 / 3.0) * VISCOSITY * delta[direction]
    for d in range(3):
        tg[d] = tg[d] - bulk
    tg[direction] = tg[direction] + 2.0 * VISCOSITY * delta[direction]
    for other in range(3):
        if other != direction:
            slot = {1: 3, 2: 4, 3: 5}[direction + other]
            tg[slot] = tg[slot] + VISCOSITY * delta[other]
    tg[6 + direction] = tg[6 + direction] + CONDUCT * delta[3]
    return tg


def flux_of(tg, vel, direction):
    t = [
        (tg[0], tg[3], tg[4]),
        (tg[3], tg[1], tg[5]),
        (tg[4], tg[5], tg[2]),
    ][direction]
    work = vel[0] * t[0] + vel[1] * t[1] + vel[2] * t[2] + tg[6 + direction]
    return [t[0], t[1], t[2], work]


def ghost_lift(flux, vel, delta, direction, lift_direction):
    zero = jnp.zeros_like(delta[0])
    tg = add_lift([zero] * 9, delta, lift_direction)
    change = flux_of(tg, vel, direction)
    return [f + d for f, d in zip(flux, change)]


def pack_faces(fields, table_of):
    total = None
    for j in range(3):
        value = move(halves(stack([fields[3 * s + j] for s in range(3)])), table_of(j))
        total = value if total is None else total + value
    return total


def edge_rows(fields, table_of):
    edges = move(halves(stack([fields[0], fields[3]])), table_of(0))
    first = edges[0:48]
    for j in (1, 2):
        first = first + move(halves(fields[j]), table_of(j))
    return stack([first, edges[48:96]])


def euler(rho, vel, pres, direction):
    normal = vel[direction]
    mass = rho * normal
    square = vel[0] * vel[0] + vel[1] * vel[1] + vel[2] * vel[2]
    energy = pres * (1.0 / (GAMMA - 1.0)) + 0.5 * rho * square
    flux = [mass] + [mass * v for v in vel] + [(energy + pres) * normal]
    flux[1 + direction] = flux[1 + direction] + pres
    state = [rho, rho * vel[0], rho * vel[1], rho * vel[2], energy]
    return (flux, state)


def face_terms(own, out, direction, sig, scale):
    rho, vel, temp = own
    rho_out, vel_out, temp_out = out
    flux, state = euler(rho, vel, rho * temp, direction)
    flux_out, state_out = euler(rho_out, vel_out, rho_out * temp_out, direction)
    speed = jnp.maximum(
        jnp.abs(vel[direction]) + jnp.sqrt(GAMMA * temp),
        jnp.abs(vel_out[direction]) + jnp.sqrt(GAMMA * temp_out),
    )
    speed = speed * jnp.abs(sig)
    return [
        (HALF_W * scale) * (sig * (fo - fi) + speed * (so - si))
        for fi, fo, si, so in zip(flux, flux_out, state, state_out)
    ]


def period_of(size):
    return 32 if size % 32 == 0 else size


def sends_late():
    period = period_of(lax.axis_size("gx"))
    return lax.rem(lax.axis_index("gx"), period) == period - 1


def is_device(gx, gz):
    return jnp.logical_and(lax.axis_index("gx") == gx, lax.axis_index("gz") == gz)


def hears_late():
    first = lax.rem(lax.axis_index("gx"), period_of(lax.axis_size("gx"))) == 0
    return jnp.logical_or(first, is_device(1, 0))


def ends_late():
    period = period_of(lax.axis_size("gx"))
    pair = lax.rem(lax.axis_index("gx"), period) >= period - 2
    return jnp.logical_or(pair, is_device(0, 0))


def parity_of(axis):
    return lax.rem(lax.axis_index(axis), 2) == 0


def first_kernel(state_hbm, mask_hbm, h_hbm, coef_hbm, st_ref, aux_ref, dh_ref, dl_ref, sw_ref, tg_ref,
                 even_ref, odd_ref, turn_1, turn_2, turn_3, edge_ref, upper_ref, state_buf, mask_buf, h_buf, coef_buf, face_buf, sems):
    copies = [
        pltpu.make_async_copy(src, dst, sems.at[i])
        for i, (src, dst) in enumerate(
            ((coef_hbm, coef_buf), (state_hbm, state_buf), (mask_hbm, mask_buf), (h_hbm, h_buf))
        )
    ]
    for copy in copies:
        copy.start()
    lanes = Lanes()
    for d in range(3):
        sw_ref[d] = swap_table(lanes, d)
    copies[0].wait()
    for d in range(3):
        high, low = halves(deriv_table(lanes, coef_buf, d))
        dh_ref[d] = high
        dl_ref[d] = low
    for copy in copies[1:]:
        copy.wait()
    for i in range(5):
        st_ref[i] = read_rows(state_buf, i)
    rho, _, _, vel, _, temp, _ = load_prims(st_ref)
    wall_lo, wall_hi = walls_of(mask_buf, lanes)
    sy = scale_y(h_buf, lanes)
    slot = lax.broadcasted_iota(jnp.int32, (ROWS, 128), 1)
    aux_ref[...] = jnp.where(
        slot == 0,
        jnp.where(wall_lo, 1.0, 0.0),
        jnp.where(slot == 1, jnp.where(wall_hi, 1.0, 0.0), sy),
    )
    own = vel + [temp]
    keep = jnp.logical_and(lanes.ghost_x, lanes.ghost_z)
    edges = edge_rows([jnp.where(keep, f, 0.0) for f in own], edge_pack_table)
    edge_ref[...] = stack([edges[24:48], edges[72:96]])
    pair = halves(stack(own))
    scales = (SCALE_X, sy, SCALE_Z)
    grads = []
    for d in range(3):
        slope = rows_of(derive(pair, dh_ref[d], dl_ref[d]), 4)
        swapped = rows_of(move(pair, sw_ref[d]), 4)
        grad = []
        for i in range(4):
            if d == 0:
                out = inner_x(swapped[i], own[i], lanes)
            elif d == 2:
                out = inner_z(swapped[i], own[i], lanes)
            else:
                sign = 1.0 if i == 3 else -1.0
                out = inner_y(swapped[i], own[i], lanes, wall_lo, wall_hi, sign)
            grad.append(scales[d] * (slope[i] + (HALF_W * lanes.sig[d]) * (own[i] - out)))
        grads.append(grad)
    tg = stress(grads)
    for i in range(9):
        tg_ref[i] = tg[i]
    fields = [rho] + own + flux_of(tg, vel, 0)
    fields = [jnp.where(lanes.hi[0], f[24:48], 0.0) for f in fields]
    upper_ref[...] = pack_faces(fields, lambda j: pack_table(0, j))
    fields = [rho] + own + flux_of(tg, vel, 2)
    fields = [jnp.where(lanes.ghost_z, f, 0.0) for f in fields]
    face_buf[...] = pack_faces(fields, lambda j: pack_table(2, j))
    down = face_buf[pl.ds(0, 72, stride=2), :]
    up = face_buf[pl.ds(1, 72, stride=2), :]
    even = parity_of("gz")
    even_ref[...] = jnp.where(even, up, down)
    odd_ref[...] = jnp.where(even, down, up)
    for ref, turn in zip((turn_1, turn_2, turn_3), turns_of(lax.axis_size("gz"))):
        ref[...] = jnp.where(among(lax.axis_index("gz"), turn), up, down)


def aux_of(aux_ref):
    return (aux_ref[:, 0:1] > 0.5, aux_ref[:, 1:2] > 0.5, aux_ref[:, 2:3])


def volume(reg_hbm, state_ref, aux_ref, dh_ref, dl_ref, sw_ref, out_ref, reg_buf, sem):
    copy = pltpu.make_async_copy(reg_hbm, reg_buf, sem)
    copy.start()
    lanes = Lanes()
    rho, mom, energy, vel, pres, temp, inv = load_prims(state_ref)
    wall_lo, wall_hi, sy = aux_of(aux_ref)
    scales = (SCALE_X, sy, SCALE_Z)
    spec = energy * inv
    common = halves(stack([rho] + vel + [pres, spec] + mom + [energy]))
    swap_pair = halves(stack([rho] + vel + [temp]))
    others = vel + [spec]
    dens = mom + [energy]
    own = [rho] + vel + [temp]
    total = [None] * 5
    for d in range(3):
        normal = vel[d]
        mine = [pres * normal] + [normal * o for o in others] + [normal * m for m in dens]
        base = rows_of(derive(common, dh_ref[d], dl_ref[d]), 10)
        rest = rows_of(derive(halves(stack(mine)), dh_ref[d], dl_ref[d]), 9)
        d_rho, d_pres, d_work = (base[0], base[4], rest[0])
        d_others = base[1:4] + [base[5]]
        d_dens = base[6:10]
        d_norm, d_mass = (base[1 + d], base[6 + d])
        mass = mom[d]
        parts = [0.5 * (rho * d_norm + normal * d_rho + d_mass)]
        for m in range(4):
            value = 0.25 * (
                rest[5 + m]
                + rho * rest[1 + m]
                + normal * d_dens[m]
                + others[m] * (d_mass + rho * d_norm + normal * d_rho)
                + mass * d_others[m]
            )
            if m == d:
                value = value + d_pres
            if m == 3:
                value = value + 0.5 * (pres * d_norm + normal * d_pres + d_work)
            parts.append(value)
        swapped = rows_of(move(swap_pair, sw_ref[d]), 5)
        outs = []
        for i in range(5):
            if d == 0:
                outs.append(inner_x(swapped[i], own[i], lanes))
            elif d == 2:
                outs.append(inner_z(swapped[i], own[i], lanes))
            else:
                sign = -1.0 if i in (1, 2, 3) else 1.0
                outs.append(inner_y(swapped[i], own[i], lanes, wall_lo, wall_hi, sign))
        faces = face_terms(
            (rho, vel, temp), (outs[0], outs[1:4], outs[4]), d, lanes.sig[d], scales[d]
        )
        for i in range(5):
            value = faces[i] - scales[d] * parts[i]
            total[i] = value if d == 0 else total[i] + value
    copy.wait()
    for i in range(5):
        out_ref[i] = SECTION_A * read_rows(reg_buf, i) + TIME_STEP * total[i]


def starts_late():
    return jnp.logical_or(sends_late(), is_device(0, 0))


def volume_kernel(reg_hbm, state_ref, aux_ref, dh_ref, dl_ref, sw_ref,
                  out_ref, uz_ref, px_ref, ep_ref, ux_ref, eu_ref, reg_buf, sem):
    lanes = Lanes()
    for j in range(3):
        uz_ref[j] = unpack_table(lanes, 2, j)
        px_ref[j] = pack_table(0, j)
        ep_ref[j] = edge_pack_table(j)
        ux_ref[j] = unpack_table(lanes, 0, j)
        eu_ref[j] = edge_unpack_table(lanes, j)

    @pl.when(jnp.logical_not(starts_late()))
    def _():
        volume(reg_hbm, state_ref, aux_ref, dh_ref, dl_ref, sw_ref, out_ref, reg_buf, sem)


def sides_of(from_even, from_odd, axis):
    even = parity_of(axis)
    return (jnp.where(even, from_odd, from_even), jnp.where(even, from_even, from_odd))


def unpack_faces(pair, table_ref, keep):
    fields = [None] * 9
    for j in range(3):
        for s, value in enumerate(rows_of(move(pair, table_ref[j]), 3)):
            fields[3 * s + j] = jnp.where(keep, value, 0.0)
    return fields


def complete_z(lanes, state_ref, tg_ref, lower, upper, uz_ref, px_ref, ep_ref, face_buf):
    rho, _, _, vel, _, temp, _ = load_prims(state_ref)
    own = vel + [temp]
    face_buf[pl.ds(0, 72, stride=2), :] = lower
    face_buf[pl.ds(1, 72, stride=2), :] = upper
    ghost = unpack_faces(halves(face_buf[...]), uz_ref, lanes.ghost_z)
    weight = jnp.where(lanes.ghost_z, (SCALE_Z * HALF_W) * lanes.sig[2], 0.0)
    delta = [weight * (o - g) for o, g in zip(own, ghost[1:5])]
    tg = add_lift([tg_ref[i] for i in range(9)], delta, 2)
    flux = ghost_lift(ghost[5:9], ghost[1:4], delta, 2, 2)
    fields = [rho] + own + flux_of(tg, vel, 0)
    fields = [jnp.where(lanes.ghost_x, f, 0.0) for f in fields]
    total = pack_faces(fields, lambda j: px_ref[j])
    edges = edge_rows([jnp.where(lanes.ghost_x, g, 0.0) for g in ghost[1:5]], lambda j: ep_ref[j])
    total = total + stack([edges, jnp.zeros((ROWS, 128), F32)])
    down = stack([total[48 * s : 48 * s + 24] for s in range(3)])
    up = stack([total[48 * s + 24 : 48 * s + 48] for s in range(3)])
    return (own, tg, ghost[:5] + flux, up, down)


def second_kernel(state_ref, tg_ref, turn_1, turn_2, turn_3, uz_ref, px_ref, ep_ref,
                  tgo_ref, gz_ref, even_out, odd_out, face_buf):
    @pl.when(jnp.logical_not(sends_late()))
    def _():
        lower, upper = (jnp.zeros((72, 128), F32), jnp.zeros((72, 128), F32))
        for ref, turn in zip((turn_1, turn_2, turn_3), turns_of(lax.axis_size("gz"))):
            above = among(lax.axis_index("gz"), turn)
            upper = upper + jnp.where(above, ref[...], 0.0)
            lower = lower + jnp.where(above, 0.0, ref[...])
        _, tg, ghost, up, down = complete_z(Lanes(), state_ref, tg_ref, lower, upper, uz_ref, px_ref, ep_ref, face_buf)
        for i in range(9):
            tgo_ref[i] = tg[i]
            gz_ref[i] = ghost[i]
        even = parity_of("gx")
        even_out[...] = jnp.where(even, up, down)
        odd_out[...] = jnp.where(even, down, up)


def third_kernel(state_ref, tg_first_ref, tg_ref, gz_ref, mine_ref, even_ref, odd_ref,
                 uz_ref, px_ref, ep_ref, tgo_ref, gzo_ref, even_out, face_buf):
    late = sends_late()

    @pl.when(late)
    def _():
        lanes = Lanes()
        lower, upper = sides_of(even_ref[...], odd_ref[...], "gz")
        _, tg, ghost, up, down = complete_z(
            lanes, state_ref, tg_first_ref, lower, upper, uz_ref, px_ref, ep_ref, face_buf
        )
        for i in range(9):
            tgo_ref[i] = tg[i]
            gzo_ref[i] = ghost[i]
        even_out[...] = jnp.where(parity_of("gx"), up, down)

    @pl.when(jnp.logical_not(late))
    def _():
        tgo_ref[...] = tg_ref[...]
        gzo_ref[...] = gz_ref[...]
        even_out[...] = mine_ref[...]


def finish(from_even, vol_ref, state_ref, tg_ref, gz_ref, aux_ref, odd_ref, up_ref,
           below_ref, above_ref, dh_ref, dl_ref, sw_ref, ux_ref, eu_ref,
           state_hbm, reg_hbm, state_out, reg_out, sems):
    lanes = Lanes()
    rho, mom, energy, vel, _, temp, _ = load_prims(state_ref)
    wall_lo, wall_hi, sy = aux_of(aux_ref)
    scales = (SCALE_X, sy, SCALE_Z)
    own = vel + [temp]
    lower, upper = sides_of(from_even, odd_ref[...], "gx")
    lower = lower + up_ref[...]
    late = hears_late()
    row = lax.broadcasted_iota(jnp.int32, (48, 128), 0)
    slot = lax.broadcasted_iota(jnp.int32, (48, 128), 1)
    direct = jnp.where(row % 2 == 0, shift(below_ref[...], -1), shift(above_ref[...], 1))
    edge_slot = jnp.where(late, slot, 0) >= 108
    lower = stack([jnp.where(edge_slot, direct, lower[0:48]), lower[48:72]])
    pair = halves(
        stack([side[24 * s : 24 * s + 24] for s in range(3) for side in (lower, upper)])
    )
    ghost_x = unpack_faces(pair, ux_ref, lanes.ghost_x)
    edge = [rows_of(move(pair, eu_ref[j]), 3) for j in range(3)]
    edge = [edge[0][0], edge[1][0], edge[2][0], edge[0][1]]
    ghost_z = [gz_ref[i] for i in range(9)]
    weight = jnp.where(lanes.ghost_x, (SCALE_X * HALF_W) * lanes.sig[0], 0.0)
    delta = [weight * (o - g) for o, g in zip(own, ghost_x[1:5])]
    tg = add_lift([tg_ref[i] for i in range(9)], delta, 0)
    flux_x = ghost_lift(ghost_x[5:9], ghost_x[1:4], delta, 0, 0)
    weight = jnp.where(lanes.ghost_z, weight, 0.0)
    edge_delta = [weight * (g - e) for g, e in zip(ghost_z[1:5], edge)]
    flux_z = ghost_lift(ghost_z[5:9], ghost_z[1:4], edge_delta, 2, 0)
    weight = jnp.where(lanes.ghost_z, (SCALE_Z * HALF_W) * lanes.sig[2], 0.0)
    weight = jnp.where(jnp.logical_and(lanes.ghost_x, jnp.where(late, lanes.a, 1) == 0), weight, 0.0)
    edge_delta = [weight * (g - e) for g, e in zip(ghost_x[1:5], edge)]
    flux_x = ghost_lift(flux_x, ghost_x[1:4], edge_delta, 0, 2)
    total = [0.0] * 5
    for d, ghost, keep in ((0, ghost_x, lanes.ghost_x), (2, ghost_z, lanes.ghost_z)):
        out = [jnp.where(keep, g, o) for g, o in zip(ghost[:5], [rho] + own)]
        faces = face_terms(
            (rho, vel, temp), (out[0], out[1:4], out[4]), d, lanes.sig[d], scales[d]
        )
        total = [t + f for t, f in zip(total, faces)]
    for d in range(3):
        flux = flux_of(tg, vel, d)
        pair = halves(stack(flux))
        slope = rows_of(derive(pair, dh_ref[d], dl_ref[d]), 4)
        swapped = rows_of(move(pair, sw_ref[d]), 4)
        for i in range(4):
            if d == 0:
                out = jnp.where(lanes.ghost_x, flux_x[i], inner_x(swapped[i], flux[i], lanes))
            elif d == 2:
                out = jnp.where(lanes.ghost_z, flux_z[i], inner_z(swapped[i], flux[i], lanes))
            else:
                out = inner_y(swapped[i], flux[i], lanes, wall_lo, wall_hi, 1.0)
            total[i + 1] = total[i + 1] + scales[d] * (
                slope[i] + (HALF_W * lanes.sig[d]) * (flux[i] - out)
            )
    for i, field in enumerate([rho] + mom + [energy]):
        reg = vol_ref[i] + TIME_STEP * total[i]
        write_rows(reg_out, i, reg)
        write_rows(state_out, i, field + SECTION_B * reg)
    copies = [
        pltpu.make_async_copy(reg_out, reg_hbm, sems.at[0]),
        pltpu.make_async_copy(state_out, state_hbm, sems.at[1]),
    ]
    for copy in copies:
        copy.start()
    for copy in copies:
        copy.wait()


def last_a_kernel(even_ref, vol_ref, *refs):
    @pl.when(jnp.logical_not(ends_late()))
    def _():
        finish(even_ref[...], vol_ref, *refs)


def last_b_kernel(state_in, reg_in, register_hbm, even_a_ref, even_b_ref, vol_ref, state_ref, tg_ref, gz_ref,
                  aux_ref, odd_ref, up_ref, below_ref, above_ref, dh_ref, dl_ref, sw_ref, *refs):
    vol_buf, reg_buf, sem = refs[-3:]

    @pl.when(ends_late())
    def _():
        @pl.when(starts_late())
        def _():
            volume(register_hbm, state_ref, aux_ref, dh_ref, dl_ref, sw_ref, vol_buf, reg_buf, sem)

        @pl.when(jnp.logical_not(starts_late()))
        def _():
            vol_buf[...] = vol_ref[...]

        finish(
            even_a_ref[...] + even_b_ref[...], vol_buf, state_ref, tg_ref, gz_ref, aux_ref, odd_ref,
            up_ref, below_ref, above_ref, dh_ref, dl_ref, sw_ref, *refs[:-3],
        )


def field_shape(count):
    return jax.ShapeDtypeStruct((count, ROWS, NODES), F32)


LIMIT = 20 * 1024 * 1024
FACE = jax.ShapeDtypeStruct((72, 128), F32)


def call(kernel, outs, flops, **more):
    return pl.pallas_call(
        kernel,
        out_shape=outs,
        compiler_params=pltpu.CompilerParams(vmem_limit_bytes=LIMIT),
        cost_estimate=pl.CostEstimate(flops=flops, bytes_accessed=2_000_000, transcendentals=0),
        **more,
    )


def send(value, partner):
    nx, nz = (lax.axis_size("gx"), lax.axis_size("gz"))
    pairs = []
    for i in range(nx):
        for j in range(nz):
            to = partner(i, j)
            if to is not None:
                pairs.append((i * nz + j, (to[0] % nx) * nz + to[1] % nz))
    return lax.ppermute(value, ("gx", "gz"), pairs)


def odd_partner(i):
    return i + 1 if i % 2 else i - 1


def turns_of(size):
    return {8: ((1, 3, 6), (2, 4, 7), (0, 5)), 4: ((1,), (3,), (0, 2))}[size]


def among(position, members):
    found = position == members[0]
    for member in members[1:]:
        found = jnp.logical_or(found, position == member)
    return found


def shards(state, register, heights, solid_wall_mask):
    coef = jnp.asarray(coefficients())
    h = heights.reshape(1, 12)

    def rows(array):
        return jnp.transpose(array, (0, 2, 3, 1, 4))

    def unrows(array):
        return jnp.transpose(array, (0, 3, 1, 2, 4))

    reg = pltpu.with_memory_space_constraint(rows(register), pltpu.HBM)
    whole = jax.ShapeDtypeStruct((2, 5, 12, 2, NODES), F32)
    table = jax.ShapeDtypeStruct((3, NODES, NODES), BF16)
    aux_shape = jax.ShapeDtypeStruct((ROWS, 128), F32)
    hbm = pl.BlockSpec(memory_space=pltpu.HBM)
    edge_shape = jax.ShapeDtypeStruct((48, 128), F32)
    st, aux, dh, dl, sw, tg_first, even_z, odd_z, *turns_z, edge, up_x = call(
        first_kernel,
        (field_shape(5), aux_shape, table, table, table, field_shape(9), *[FACE] * 5, edge_shape, FACE),
        10**8,
        in_specs=[hbm] * 4,
        scratch_shapes=[
            pltpu.VMEM((2, 5, 12, 2, NODES), F32),
            pltpu.VMEM((2, 2, 11), jnp.int32),
            pltpu.VMEM((1, 12), F32),
            pltpu.VMEM((18, NODES), F32),
            pltpu.VMEM((144, 128), F32),
            pltpu.SemaphoreType.DMA((4,)),
        ],
    )(*[pltpu.with_memory_space_constraint(v, pltpu.HBM) for v in (rows(state), solid_wall_mask, h, coef)])
    period = period_of(lax.axis_size("gx"))
    late = lambda i: i % period == period - 1
    ok = lambda flag, to: to if flag else None
    origin = lambda i, j: i == 0 and j == 0
    beside = lambda i, j: i == 1 and j == 0
    last_z = lax.axis_size("gz") - 1
    below = send(edge, lambda i, j: ok(late(i) or (i == 0 and j == last_z), (i + 1, j + 1)))
    above = send(edge, lambda i, j: ok(late(i) or (i == 0 and j == 1), (i + 1, j - 1)))
    up_x = send(up_x, lambda i, j: ok(late(i) or origin(i, j), (i + 1, j)))
    za = []
    for n, turn in enumerate(turns_of(last_z + 1)):
        to = {j: (j + 1) % (last_z + 1) for j in turn}
        to.update({v: k for k, v in to.items()})
        za.append(send(turns_z[n], lambda i, j: ok(j in to and not late(i), (i, to.get(j)))))
    pack = jax.ShapeDtypeStruct((3, NODES, 128), BF16)
    unpack = jax.ShapeDtypeStruct((3, 128, NODES), BF16)
    vmem = pl.BlockSpec(memory_space=pltpu.VMEM)
    block = pltpu.VMEM((2, 5, 12, 2, NODES), F32)
    vol, uz, px, ep, ux, eu = call(
        volume_kernel,
        (field_shape(5), unpack, pack, pack, unpack, unpack),
        10**6,
        in_specs=[hbm] + [vmem] * 5,
        scratch_shapes=[block, pltpu.SemaphoreType.DMA],
    )(reg, st, aux, dh, dl, sw)
    face_buf = [pltpu.VMEM((144, 128), F32)]
    tg, gz, even_x, odd_x = call(
        second_kernel, (field_shape(9), field_shape(9), FACE, FACE), 10**8, scratch_shapes=face_buf
    )(st, tg_first, *za, uz, px, ep)
    early = lambda i: not (late(i) or late(i ^ 1))
    apart = lambda i, j: i < 2 and j == 0
    xa_even = send(even_x, lambda i, j: ok(early(i) and not apart(i, j), (i ^ 1, j)))
    x_odd = send(odd_x, lambda i, j: ok(not late(i), (odd_partner(i), j)))
    zb_even = send(even_z, lambda i, j: ok(late(i), (i, j ^ 1)))
    zb_odd = send(odd_z, lambda i, j: ok(late(i), (i, odd_partner(j))))
    tg, gz, even_x = call(
        third_kernel, (field_shape(9), field_shape(9), FACE), 10**8, scratch_shapes=face_buf
    )(st, tg_first, tg, gz, even_x, zb_even, zb_odd, uz, px, ep)
    rest = (vol, st, tg, gz, aux, x_odd, up_x, below, above, dh, dl, sw, ux, eu)
    buffers = [block, block, pltpu.SemaphoreType.DMA((2,))]
    outs = call(
        last_a_kernel, (whole, whole), 10**8, in_specs=[vmem] * 15, out_specs=[hbm, hbm], scratch_shapes=buffers
    )(xa_even, *rest)
    xb_even = send(even_x, lambda i, j: ok(not early(i) or beside(i, j), (i ^ 1, j)))
    state_next, reg_next = call(
        last_b_kernel,
        (whole, whole),
        10**8,
        in_specs=[hbm] * 3 + [vmem] * 16,
        out_specs=[hbm, hbm],
        scratch_shapes=buffers + [pltpu.VMEM((5, ROWS, NODES), F32), block, pltpu.SemaphoreType.DMA],
        input_output_aliases={0: 0, 1: 1},
    )(*outs, reg, xa_even, xb_even, *rest)
    return (unrows(state_next), unrows(reg_next))


def solution(mesh):
    spec = P("gx", "gz", None, None, None)

    return jax.shard_map(
        shards,
        mesh=mesh,
        in_specs=(spec, spec, P(), P("gx", "gz", None)),
        out_specs=(spec, spec),
        check_vma=False,
    )
```

```python
import functools
import math

import jax
import jax.numpy as jnp
import numpy as np
from jax import lax
from jax.experimental import pallas as pl
from jax.experimental.pallas import tpu as pltpu
from jax.sharding import PartitionSpec as P


GAMMA = 1.4
VISCOSITY = 0.001
CONDUCT = 0.001 * 1.4 / (0.4 * 0.72)
SCALE_X = 2.0 / 0.2
SCALE_Z = 2.0 / 0.15
TIME_STEP = 0.004
SECTION_A = -0.4178904745
SECTION_B = 0.3792103129
HALF_W = 7.5


ROWS, NODES = (48, 216)
F32, BF16 = (jnp.float32, jnp.bfloat16)


def node_matrix():
    root = math.sqrt(7.0)
    outer = math.sqrt(1.0 / 3.0 + 2.0 * root / 21.0)
    inner = math.sqrt(1.0 / 3.0 - 2.0 * root / 21.0)
    points = np.array([-1.0, -outer, -inner, inner, outer, 1.0])
    barycen = np.array(
        [1.0 / np.prod([points[i] - points[j] for j in range(6) if j != i]) for i in range(6)]
    )
    matrix = np.zeros((6, 6))
    for i in range(6):
        for j in range(6):
            if j != i:
                matrix[i, j] = barycen[j] / barycen[i] / (points[i] - points[j])
        matrix[i, i] = -np.sum(matrix[i])
    return matrix


STRIDE = (36, 6, 1)


def hot(sources, depth):
    rows = lax.broadcasted_iota(jnp.int32, (depth, sources[0].shape[1]), 0)
    found = rows == sources[0]
    for source in sources[1:]:
        found = jnp.logical_or(found, rows == source)
    return jnp.where(found, 1.0, 0.0).astype(BF16)


def slot_lane(first, width):
    lane = lax.broadcasted_iota(jnp.int32, (1, 128), 1) - first
    return jnp.where(jnp.logical_and(lane >= 0, lane < width), lane, -1000)


def pack_table(d, j):
    node = slot_lane(36 * j, 36) * (1 if d == 0 else 6)
    return hot([node, node + 5 * STRIDE[d]], NODES)


def unpack_table(lanes, d, j):
    node = lax.broadcasted_iota(jnp.int32, (1, NODES), 1)
    face = (node % 36) if d == 0 else node // 6
    return hot([jnp.where(lanes.face[d], 36 * j + face, -1)], 128)


def edge_pack_table(j):
    node = 6 * slot_lane(108 + 6 * j, 6)
    return hot([node, node + 5, node + 180, node + 185], NODES)


def edge_unpack_table(lanes, j):
    edge = jnp.logical_and(lanes.face[0], lanes.face[2])
    return hot([jnp.where(edge, 108 + 6 * j + lanes.place[1], -1)], 128)


def swap_table(lanes, d):
    lane = lax.broadcasted_iota(jnp.int32, (1, NODES), 1)
    step = 5 * STRIDE[d]
    return hot(
        [jnp.where(lanes.lo[d], lane + step, jnp.where(lanes.hi[d], lane - step, -1))], NODES
    )


def deriv_table(lanes, matrix, d):
    lane = lax.broadcasted_iota(jnp.int32, (1, NODES), 1)
    base = lane - STRIDE[d] * lanes.place[d]
    rows = lax.broadcasted_iota(jnp.int32, (NODES, NODES), 0) - base
    table = jnp.zeros((NODES, NODES), F32)
    for j in range(6):
        line = jnp.zeros((1, NODES), F32)
        for i in range(6):
            line = jnp.where(lanes.place[d] == i, float(np.float32(matrix[i, j])), line)
        table = jnp.where(rows == STRIDE[d] * j, line, table)
    return table


def halves(value):
    high = value.astype(BF16)
    return (high, (value - high.astype(F32)).astype(BF16))


def dot(a, b):
    return jnp.dot(a, b, preferred_element_type=F32)


def derive(pair, dh, dl):
    return dot(pair[0], dh) + (dot(pair[1], dh) + dot(pair[0], dl))


def move(pair, table):
    return dot(pair[0], table) + dot(pair[1], table)


def stack(fields):
    return jnp.concatenate(fields, axis=0)


def rows_of(value, count, size=ROWS):
    return [value[i * size : (i + 1) * size] for i in range(count)]


class Lanes:
    def __init__(self):
        lane = lax.broadcasted_iota(jnp.int32, (1, NODES), 1)
        row = lax.broadcasted_iota(jnp.int32, (ROWS, 1), 0)
        self.a, self.c = (row // 24, row % 2)
        self.k = (row % 24) // 2
        place = (lane // 36, lane // 6 % 6, lane % 6)
        self.place = place
        self.lo = [p == 0 for p in place]
        self.hi = [p == 5 for p in place]
        self.sig = [
            jnp.where(p == 0, 1.0, 0.0) + jnp.where(p == 5, -1.0, 0.0) for p in place
        ]
        self.face = [jnp.logical_or(lo, hi) for lo, hi in zip(self.lo, self.hi)]
        self.ghost_x = jnp.logical_or(
            jnp.logical_and(self.a == 0, self.lo[0]), jnp.logical_and(self.a == 1, self.hi[0])
        )
        self.ghost_z = jnp.logical_or(
            jnp.logical_and(self.c == 0, self.lo[2]), jnp.logical_and(self.c == 1, self.hi[2])
        )


def read_rows(ref, field):
    return stack([ref[a, field].reshape(24, NODES) for a in range(2)])


def load_prims(state_ref):
    rho = state_ref[0]
    inv = 1.0 / rho
    mom = [state_ref[1], state_ref[2], state_ref[3]]
    vel = [m * inv for m in mom]
    energy = state_ref[4]
    pres = (GAMMA - 1.0) * (
        energy - 0.5 * (mom[0] * vel[0] + mom[1] * vel[1] + mom[2] * vel[2])
    )
    return (rho, mom, energy, vel, pres, pres * inv, inv)


def walls_of(mask_ref, lanes):
    spread = jnp.zeros((ROWS, 11), jnp.int32)
    for a in range(2):
        for c in range(2):
            here = jnp.logical_and(lanes.a == a, lanes.c == c)
            spread = jnp.where(here, mask_ref[a, c : c + 1, :], spread)
    column = lax.broadcasted_iota(jnp.int32, (ROWS, 11), 1)
    solid = jnp.where(spread == 1, 1.0, 0.0)
    low = jnp.sum(jnp.where(column == lanes.k - 1, solid, 0.0), axis=1, keepdims=True)
    high = jnp.sum(jnp.where(column == lanes.k, solid, 0.0), axis=1, keepdims=True)
    return (
        jnp.logical_or(low > 0.5, lanes.k == 0),
        jnp.logical_or(high > 0.5, lanes.k == 11),
    )


def scale_y(h_ref, lanes):
    column = lax.broadcasted_iota(jnp.int32, (ROWS, 12), 1)
    own = jnp.where(column == lanes.k, h_ref[0:1, :], 0.0)
    return 2.0 / jnp.sum(own, axis=1, keepdims=True)


def shift(value, by):
    return pltpu.roll(value, by % value.shape[0], 0)


def inner_x(swapped, own, lanes):
    other = stack([swapped[24:48], swapped[0:24]])
    return jnp.where(jnp.logical_and(lanes.face[0], jnp.logical_not(lanes.ghost_x)), other, own)


def inner_z(swapped, own, lanes):
    other = jnp.where(lanes.lo[2], shift(swapped, 1), shift(swapped, -1))
    return jnp.where(jnp.logical_and(lanes.face[2], jnp.logical_not(lanes.ghost_z)), other, own)


def inner_y(swapped, own, lanes, wall_lo, wall_hi, sign):
    other = jnp.where(lanes.lo[1], shift(swapped, 2), shift(swapped, -2))
    solid = jnp.logical_or(
        jnp.logical_and(wall_lo, lanes.lo[1]), jnp.logical_and(wall_hi, lanes.hi[1])
    )
    return jnp.where(lanes.face[1], jnp.where(solid, sign * own, other), own)


def stress(grads):
    gx, gy, gz = grads
    third = (2.0 / 3.0) * VISCOSITY * (gx[0] + gy[1] + gz[2])
    return [
        2.0 * VISCOSITY * gx[0] - third,
        2.0 * VISCOSITY * gy[1] - third,
        2.0 * VISCOSITY * gz[2] - third,
        VISCOSITY * (gx[1] + gy[0]),
        VISCOSITY * (gx[2] + gz[0]),
        VISCOSITY * (gy[2] + gz[1]),
        CONDUCT * gx[3],
        CONDUCT * gy[3],
        CONDUCT * gz[3],
    ]


def add_lift(tg, delta, direction):
    tg = list(tg)
    bulk = (2.0 / 3.0) * VISCOSITY * delta[direction]
    for d in range(3):
        tg[d] = tg[d] - bulk
    tg[direction] = tg[direction] + 2.0 * VISCOSITY * delta[direction]
    for other in range(3):
        if other != direction:
            slot = {1: 3, 2: 4, 3: 5}[direction + other]
            tg[slot] = tg[slot] + VISCOSITY * delta[other]
    tg[6 + direction] = tg[6 + direction] + CONDUCT * delta[3]
    return tg


def flux_of(tg, vel, direction):
    t = [
        (tg[0], tg[3], tg[4]),
        (tg[3], tg[1], tg[5]),
        (tg[4], tg[5], tg[2]),
    ][direction]
    work = vel[0] * t[0] + vel[1] * t[1] + vel[2] * t[2] + tg[6 + direction]
    return [t[0], t[1], t[2], work]


def ghost_lift(flux, vel, delta, direction, lift_direction):
    zero = jnp.zeros_like(delta[0])
    tg = add_lift([zero] * 9, delta, lift_direction)
    change = flux_of(tg, vel, direction)
    return [f + d for f, d in zip(flux, change)]


def pack_faces(fields, table_of):
    total = None
    for j in range(3):
        value = move(halves(stack([fields[3 * s + j] for s in range(3)])), table_of(j))
        total = value if total is None else total + value
    return total


def edge_rows(fields, table_of):
    edges = move(halves(stack([fields[0], fields[3]])), table_of(0))
    first = edges[0:48]
    for j in (1, 2):
        first = first + move(halves(fields[j]), table_of(j))
    return stack([first, edges[48:96]])


def euler(rho, vel, pres, direction):
    normal = vel[direction]
    mass = rho * normal
    square = vel[0] * vel[0] + vel[1] * vel[1] + vel[2] * vel[2]
    energy = pres * (1.0 / (GAMMA - 1.0)) + 0.5 * rho * square
    flux = [mass] + [mass * v for v in vel] + [(energy + pres) * normal]
    flux[1 + direction] = flux[1 + direction] + pres
    state = [rho, rho * vel[0], rho * vel[1], rho * vel[2], energy]
    return (flux, state)


def face_terms(own, out, direction, sig, scale):
    rho, vel, temp = own
    rho_out, vel_out, temp_out = out
    flux, state = euler(rho, vel, rho * temp, direction)
    flux_out, state_out = euler(rho_out, vel_out, rho_out * temp_out, direction)
    speed = jnp.maximum(
        jnp.abs(vel[direction]) + jnp.sqrt(GAMMA * temp),
        jnp.abs(vel_out[direction]) + jnp.sqrt(GAMMA * temp_out),
    )
    speed = speed * jnp.abs(sig)
    return [
        (HALF_W * scale) * (sig * (fo - fi) + speed * (so - si))
        for fi, fo, si, so in zip(flux, flux_out, state, state_out)
    ]


def period_of(size):
    return 32 if size % 32 == 0 else size


def sends_late():
    period = period_of(lax.axis_size("gx"))
    return lax.rem(lax.axis_index("gx"), period) == period - 1


def is_device(gx, gz):
    return jnp.logical_and(lax.axis_index("gx") == gx, lax.axis_index("gz") == gz)


def hears_late():
    first = lax.rem(lax.axis_index("gx"), period_of(lax.axis_size("gx"))) == 0
    return jnp.logical_or(first, is_device(1, 0))


def ends_late():
    period = period_of(lax.axis_size("gx"))
    pair = lax.rem(lax.axis_index("gx"), period) >= period - 2
    last = lax.axis_size("gz") - 1
    near = [is_device(0, 0)] + [is_device(i, j) for i in (0, 1) for j in (1, last)]
    return functools.reduce(jnp.logical_or, near, pair)


def parity_of(axis):
    return lax.rem(lax.axis_index(axis), 2) == 0


def first_kernel(state_hbm, mask_hbm, h_hbm, st_ref, aux_ref, dh_ref, dl_ref, sw_ref, tg_ref,
                 even_ref, odd_ref, turn_1, turn_2, turn_3, edge_ref, upper_ref, state_buf, mask_buf, h_buf, face_buf, sems):
    copies = [
        pltpu.make_async_copy(src, dst, sems.at[i])
        for i, (src, dst) in enumerate(
            ((state_hbm, state_buf), (mask_hbm, mask_buf), (h_hbm, h_buf))
        )
    ]
    for copy in copies:
        copy.start()
    lanes = Lanes()
    for d in range(3):
        sw_ref[d] = swap_table(lanes, d)
    matrix = node_matrix()
    for d in range(3):
        high, low = halves(deriv_table(lanes, matrix, d))
        dh_ref[d] = high
        dl_ref[d] = low
    for copy in copies:
        copy.wait()
    for i in range(5):
        st_ref[i] = read_rows(state_buf, i)
    rho, _, _, vel, _, temp, _ = load_prims(st_ref)
    wall_lo, wall_hi = walls_of(mask_buf, lanes)
    sy = scale_y(h_buf, lanes)
    slot = lax.broadcasted_iota(jnp.int32, (ROWS, 128), 1)
    aux_ref[...] = jnp.where(
        slot == 0,
        jnp.where(wall_lo, 1.0, 0.0),
        jnp.where(slot == 1, jnp.where(wall_hi, 1.0, 0.0), sy),
    )
    own = vel + [temp]
    keep = jnp.logical_and(lanes.ghost_x, lanes.ghost_z)
    edges = edge_rows([jnp.where(keep, f, 0.0) for f in own], edge_pack_table)
    edge_ref[...] = stack([edges[24:48], edges[72:96]])
    pair = halves(stack(own))
    scales = (SCALE_X, sy, SCALE_Z)
    grads = []
    for d in range(3):
        slope = rows_of(derive(pair, dh_ref[d], dl_ref[d]), 4)
        swapped = rows_of(move(pair, sw_ref[d]), 4)
        grad = []
        for i in range(4):
            if d == 0:
                out = inner_x(swapped[i], own[i], lanes)
            elif d == 2:
                out = inner_z(swapped[i], own[i], lanes)
            else:
                sign = 1.0 if i == 3 else -1.0
                out = inner_y(swapped[i], own[i], lanes, wall_lo, wall_hi, sign)
            grad.append(scales[d] * (slope[i] + (HALF_W * lanes.sig[d]) * (own[i] - out)))
        grads.append(grad)
    tg = stress(grads)
    for i in range(9):
        tg_ref[i] = tg[i]
    fields = [rho] + own + flux_of(tg, vel, 0)
    fields = [jnp.where(lanes.hi[0], f[24:48], 0.0) for f in fields]
    upper_ref[...] = pack_faces(fields, lambda j: pack_table(0, j))
    fields = [rho] + own + flux_of(tg, vel, 2)
    fields = [jnp.where(lanes.ghost_z, f, 0.0) for f in fields]
    face_buf[...] = pack_faces(fields, lambda j: pack_table(2, j))
    down = face_buf[pl.ds(0, 72, stride=2), :]
    up = face_buf[pl.ds(1, 72, stride=2), :]
    even = parity_of("gz")
    even_ref[...] = jnp.where(even, up, down)
    odd_ref[...] = jnp.where(even, down, up)
    for ref, turn in zip((turn_1, turn_2, turn_3), turns_of(lax.axis_size("gz"))):
        ref[...] = jnp.where(among(lax.axis_index("gz"), turn), up, down)


def aux_of(aux_ref):
    return (aux_ref[:, 0:1] > 0.5, aux_ref[:, 1:2] > 0.5, aux_ref[:, 2:3])


def volume(reg_hbm, state_ref, aux_ref, dh_ref, dl_ref, sw_ref, out_ref, reg_buf, sem):
    copy = pltpu.make_async_copy(reg_hbm, reg_buf, sem)
    copy.start()
    lanes = Lanes()
    rho, mom, energy, vel, pres, temp, inv = load_prims(state_ref)
    wall_lo, wall_hi, sy = aux_of(aux_ref)
    scales = (SCALE_X, sy, SCALE_Z)
    spec = energy * inv
    common = halves(stack([rho] + vel + [pres, spec] + mom + [energy]))
    swap_pair = halves(stack([rho] + vel + [temp]))
    others = vel + [spec]
    dens = mom + [energy]
    own = [rho] + vel + [temp]
    total = [None] * 5
    for d in range(3):
        normal = vel[d]
        mine = [pres * normal] + [normal * o for o in others] + [normal * m for m in dens]
        base = rows_of(derive(common, dh_ref[d], dl_ref[d]), 10)
        rest = rows_of(derive(halves(stack(mine)), dh_ref[d], dl_ref[d]), 9)
        d_rho, d_pres, d_work = (base[0], base[4], rest[0])
        d_others = base[1:4] + [base[5]]
        d_dens = base[6:10]
        d_norm, d_mass = (base[1 + d], base[6 + d])
        mass = mom[d]
        parts = [0.5 * (rho * d_norm + normal * d_rho + d_mass)]
        for m in range(4):
            value = 0.25 * (
                rest[5 + m]
                + rho * rest[1 + m]
                + normal * d_dens[m]
                + others[m] * (d_mass + rho * d_norm + normal * d_rho)
                + mass * d_others[m]
            )
            if m == d:
                value = value + d_pres
            if m == 3:
                value = value + 0.5 * (pres * d_norm + normal * d_pres + d_work)
            parts.append(value)
        swapped = rows_of(move(swap_pair, sw_ref[d]), 5)
        outs = []
        for i in range(5):
            if d == 0:
                outs.append(inner_x(swapped[i], own[i], lanes))
            elif d == 2:
                outs.append(inner_z(swapped[i], own[i], lanes))
            else:
                sign = -1.0 if i in (1, 2, 3) else 1.0
                outs.append(inner_y(swapped[i], own[i], lanes, wall_lo, wall_hi, sign))
        faces = face_terms(
            (rho, vel, temp), (outs[0], outs[1:4], outs[4]), d, lanes.sig[d], scales[d]
        )
        for i in range(5):
            value = faces[i] - scales[d] * parts[i]
            total[i] = value if d == 0 else total[i] + value
    copy.wait()
    for i in range(5):
        out_ref[i] = SECTION_A * read_rows(reg_buf, i) + TIME_STEP * total[i]


def starts_late():
    return jnp.logical_or(sends_late(), is_device(0, 0))


def volume_kernel(reg_hbm, state_ref, aux_ref, dh_ref, dl_ref, sw_ref,
                  out_ref, uz_ref, px_ref, ep_ref, ux_ref, eu_ref, reg_buf, sem):
    lanes = Lanes()
    for j in range(3):
        uz_ref[j] = unpack_table(lanes, 2, j)
        px_ref[j] = pack_table(0, j)
        ep_ref[j] = edge_pack_table(j)
        ux_ref[j] = unpack_table(lanes, 0, j)
        eu_ref[j] = edge_unpack_table(lanes, j)

    @pl.when(jnp.logical_not(starts_late()))
    def _():
        volume(reg_hbm, state_ref, aux_ref, dh_ref, dl_ref, sw_ref, out_ref, reg_buf, sem)


def sides_of(from_even, from_odd, axis):
    even = parity_of(axis)
    return (jnp.where(even, from_odd, from_even), jnp.where(even, from_even, from_odd))


def unpack_faces(pair, table_ref, keep):
    fields = [None] * 9
    for j in range(3):
        for s, value in enumerate(rows_of(move(pair, table_ref[j]), 3)):
            fields[3 * s + j] = jnp.where(keep, value, 0.0)
    return fields


def complete_z(lanes, state_ref, tg_ref, lower, upper, uz_ref, px_ref, ep_ref, face_buf):
    rho, _, _, vel, _, temp, _ = load_prims(state_ref)
    own = vel + [temp]
    face_buf[pl.ds(0, 72, stride=2), :] = lower
    face_buf[pl.ds(1, 72, stride=2), :] = upper
    ghost = unpack_faces(halves(face_buf[...]), uz_ref, lanes.ghost_z)
    weight = jnp.where(lanes.ghost_z, (SCALE_Z * HALF_W) * lanes.sig[2], 0.0)
    delta = [weight * (o - g) for o, g in zip(own, ghost[1:5])]
    tg = add_lift([tg_ref[i] for i in range(9)], delta, 2)
    flux = ghost_lift(ghost[5:9], ghost[1:4], delta, 2, 2)
    fields = [rho] + own + flux_of(tg, vel, 0)
    fields = [jnp.where(lanes.ghost_x, f, 0.0) for f in fields]
    total = pack_faces(fields, lambda j: px_ref[j])
    edges = edge_rows([jnp.where(lanes.ghost_x, g, 0.0) for g in ghost[1:5]], lambda j: ep_ref[j])
    total = total + stack([edges, jnp.zeros((ROWS, 128), F32)])
    down = stack([total[48 * s : 48 * s + 24] for s in range(3)])
    up = stack([total[48 * s + 24 : 48 * s + 48] for s in range(3)])
    return (own, tg, ghost[:5] + flux, up, down)


def second_kernel(state_ref, tg_ref, turn_1, turn_2, turn_3, uz_ref, px_ref, ep_ref,
                  tgo_ref, gz_ref, even_out, odd_out, face_buf):
    @pl.when(jnp.logical_not(sends_late()))
    def _():
        lower, upper = (jnp.zeros((72, 128), F32), jnp.zeros((72, 128), F32))
        for ref, turn in zip((turn_1, turn_2, turn_3), turns_of(lax.axis_size("gz"))):
            above = among(lax.axis_index("gz"), turn)
            upper = upper + jnp.where(above, ref[...], 0.0)
            lower = lower + jnp.where(above, 0.0, ref[...])
        _, tg, ghost, up, down = complete_z(Lanes(), state_ref, tg_ref, lower, upper, uz_ref, px_ref, ep_ref, face_buf)
        for i in range(9):
            tgo_ref[i] = tg[i]
            gz_ref[i] = ghost[i]
        even = parity_of("gx")
        even_out[...] = jnp.where(even, up, down)
        odd_out[...] = jnp.where(even, down, up)


def third_kernel(state_ref, tg_first_ref, tg_ref, gz_ref, mine_ref, even_ref, odd_ref,
                 uz_ref, px_ref, ep_ref, tgo_ref, gzo_ref, even_out, face_buf):
    late = sends_late()

    @pl.when(late)
    def _():
        lanes = Lanes()
        lower, upper = sides_of(even_ref[...], odd_ref[...], "gz")
        _, tg, ghost, up, down = complete_z(
            lanes, state_ref, tg_first_ref, lower, upper, uz_ref, px_ref, ep_ref, face_buf
        )
        for i in range(9):
            tgo_ref[i] = tg[i]
            gzo_ref[i] = ghost[i]
        even_out[...] = jnp.where(parity_of("gx"), up, down)

    @pl.when(jnp.logical_not(late))
    def _():
        tgo_ref[...] = tg_ref[...]
        gzo_ref[...] = gz_ref[...]
        even_out[...] = mine_ref[...]


def finish(from_even, vol_ref, state_ref, tg_ref, gz_ref, aux_ref, odd_ref, up_ref,
           below_ref, above_ref, dh_ref, dl_ref, sw_ref, ux_ref, eu_ref,
           state_hbm, reg_hbm, state_out, reg_out, sems):
    lanes = Lanes()
    rho, mom, energy, vel, _, temp, _ = load_prims(state_ref)
    wall_lo, wall_hi, sy = aux_of(aux_ref)
    scales = (SCALE_X, sy, SCALE_Z)
    own = vel + [temp]
    lower, upper = sides_of(from_even, odd_ref[...], "gx")
    lower = lower + up_ref[...]
    late = hears_late()
    row = lax.broadcasted_iota(jnp.int32, (48, 128), 0)
    slot = lax.broadcasted_iota(jnp.int32, (48, 128), 1)
    direct = jnp.where(row % 2 == 0, shift(below_ref[...], -1), shift(above_ref[...], 1))
    edge_slot = jnp.where(late, slot, 0) >= 108
    lower = stack([jnp.where(edge_slot, direct, lower[0:48]), lower[48:72]])
    pair = halves(
        stack([side[24 * s : 24 * s + 24] for s in range(3) for side in (lower, upper)])
    )
    ghost_x = unpack_faces(pair, ux_ref, lanes.ghost_x)
    edge = [rows_of(move(pair, eu_ref[j]), 3) for j in range(3)]
    edge = [edge[0][0], edge[1][0], edge[2][0], edge[0][1]]
    ghost_z = [gz_ref[i] for i in range(9)]
    weight = jnp.where(lanes.ghost_x, (SCALE_X * HALF_W) * lanes.sig[0], 0.0)
    delta = [weight * (o - g) for o, g in zip(own, ghost_x[1:5])]
    tg = add_lift([tg_ref[i] for i in range(9)], delta, 0)
    flux_x = ghost_lift(ghost_x[5:9], ghost_x[1:4], delta, 0, 0)
    weight = jnp.where(lanes.ghost_z, weight, 0.0)
    edge_delta = [weight * (g - e) for g, e in zip(ghost_z[1:5], edge)]
    flux_z = ghost_lift(ghost_z[5:9], ghost_z[1:4], edge_delta, 2, 0)
    weight = jnp.where(lanes.ghost_z, (SCALE_Z * HALF_W) * lanes.sig[2], 0.0)
    weight = jnp.where(jnp.logical_and(lanes.ghost_x, jnp.where(late, lanes.a, 1) == 0), weight, 0.0)
    edge_delta = [weight * (g - e) for g, e in zip(ghost_x[1:5], edge)]
    flux_x = ghost_lift(flux_x, ghost_x[1:4], edge_delta, 0, 2)
    total = [0.0] * 5
    for d, ghost, keep in ((0, ghost_x, lanes.ghost_x), (2, ghost_z, lanes.ghost_z)):
        out = [jnp.where(keep, g, o) for g, o in zip(ghost[:5], [rho] + own)]
        faces = face_terms(
            (rho, vel, temp), (out[0], out[1:4], out[4]), d, lanes.sig[d], scales[d]
        )
        total = [t + f for t, f in zip(total, faces)]
    pairs = []
    for d in range(3):
        flux = flux_of(tg, vel, d)
        pairs.append([halves(f) for f in flux])
        swapped = rows_of(move([stack(list(v)) for v in zip(*pairs[d])], sw_ref[d]), 4)
        for i in range(4):
            if d == 0:
                out = jnp.where(lanes.ghost_x, flux_x[i], inner_x(swapped[i], flux[i], lanes))
            elif d == 2:
                out = jnp.where(lanes.ghost_z, flux_z[i], inner_z(swapped[i], flux[i], lanes))
            else:
                out = inner_y(swapped[i], flux[i], lanes, wall_lo, wall_hi, 1.0)
            total[i + 1] = total[i + 1] + (scales[d] * HALF_W * lanes.sig[d]) * (flux[i] - out)
    fields = [rho] + mom + [energy]
    copies = []
    for a in range(2):
        part = slice(24 * a, 24 * a + 24)
        mine = [t[part] for t in total]
        for d in range(3):
            pair = [stack([f[part] for f in v]) for v in zip(*pairs[d])]
            slope = rows_of(derive(pair, dh_ref[d], dl_ref[d]), 4, 24)
            scale = sy[part] if d == 1 else scales[d]
            for i in range(4):
                mine[i + 1] = mine[i + 1] + scale * slope[i]
        for i in range(5):
            reg = vol_ref[i][part] + TIME_STEP * mine[i]
            reg_out[a, i] = reg.reshape(12, 2, NODES)
            state_out[a, i] = (fields[i][part] + SECTION_B * reg).reshape(12, 2, NODES)
        copies += [
            pltpu.make_async_copy(reg_out.at[a], reg_hbm.at[a], sems.at[2 * a]),
            pltpu.make_async_copy(state_out.at[a], state_hbm.at[a], sems.at[2 * a + 1]),
        ]
        for copy in copies[2 * a :]:
            copy.start()
    for copy in copies:
        copy.wait()


def last_a_kernel(even_ref, vol_ref, *refs):
    @pl.when(jnp.logical_not(ends_late()))
    def _():
        finish(even_ref[...], vol_ref, *refs)


def last_b_kernel(state_in, reg_in, register_hbm, even_a_ref, even_b_ref, vol_ref, state_ref, tg_ref, gz_ref,
                  aux_ref, odd_ref, up_ref, below_ref, above_ref, dh_ref, dl_ref, sw_ref, *refs):
    vol_buf, reg_buf, sem = refs[-3:]

    @pl.when(ends_late())
    def _():
        @pl.when(starts_late())
        def _():
            volume(register_hbm, state_ref, aux_ref, dh_ref, dl_ref, sw_ref, vol_buf, reg_buf, sem)

        @pl.when(jnp.logical_not(starts_late()))
        def _():
            vol_buf[...] = vol_ref[...]

        finish(
            even_a_ref[...] + even_b_ref[...], vol_buf, state_ref, tg_ref, gz_ref, aux_ref, odd_ref,
            up_ref, below_ref, above_ref, dh_ref, dl_ref, sw_ref, *refs[:-3],
        )


def field_shape(count):
    return jax.ShapeDtypeStruct((count, ROWS, NODES), F32)


LIMIT = 20 * 1024 * 1024
FACE = jax.ShapeDtypeStruct((72, 128), F32)


def call(kernel, outs, flops, **more):
    return pl.pallas_call(
        kernel,
        out_shape=outs,
        compiler_params=pltpu.CompilerParams(vmem_limit_bytes=LIMIT),
        cost_estimate=pl.CostEstimate(flops=flops, bytes_accessed=2_000_000, transcendentals=0),
        **more,
    )


def send(value, partner):
    nx, nz = (lax.axis_size("gx"), lax.axis_size("gz"))
    pairs = []
    for i in range(nx):
        for j in range(nz):
            to = partner(i, j)
            if to is not None:
                pairs.append((i * nz + j, (to[0] % nx) * nz + to[1] % nz))
    return lax.ppermute(value, ("gx", "gz"), pairs)


def odd_partner(i):
    return i + 1 if i % 2 else i - 1


def turns_of(size):
    return {8: ((1, 3, 6), (2, 4, 7), (0, 5)), 4: ((1,), (3,), (0, 2))}[size]


def among(position, members):
    found = position == members[0]
    for member in members[1:]:
        found = jnp.logical_or(found, position == member)
    return found


def shards(state, register, heights, solid_wall_mask):
    h = heights.reshape(1, 12)

    def rows(array):
        return jnp.transpose(array, (0, 2, 3, 1, 4))

    def unrows(array):
        return jnp.transpose(array, (0, 3, 1, 2, 4))

    reg = pltpu.with_memory_space_constraint(rows(register), pltpu.HBM)
    whole = jax.ShapeDtypeStruct((2, 5, 12, 2, NODES), F32)
    table = jax.ShapeDtypeStruct((3, NODES, NODES), BF16)
    aux_shape = jax.ShapeDtypeStruct((ROWS, 128), F32)
    hbm = pl.BlockSpec(memory_space=pltpu.HBM)
    edge_shape = jax.ShapeDtypeStruct((48, 128), F32)
    st, aux, dh, dl, sw, tg_first, even_z, odd_z, *turns_z, edge, up_x = call(
        first_kernel,
        (field_shape(5), aux_shape, table, table, table, field_shape(9), *[FACE] * 5, edge_shape, FACE),
        10**8,
        in_specs=[hbm] * 3,
        scratch_shapes=[
            pltpu.VMEM((2, 5, 12, 2, NODES), F32),
            pltpu.VMEM((2, 2, 11), jnp.int32),
            pltpu.VMEM((1, 12), F32),
            pltpu.VMEM((144, 128), F32),
            pltpu.SemaphoreType.DMA((3,)),
        ],
    )(*[pltpu.with_memory_space_constraint(v, pltpu.HBM) for v in (rows(state), solid_wall_mask, h)])
    period = period_of(lax.axis_size("gx"))
    late = lambda i: i % period == period - 1
    ok = lambda flag, to: to if flag else None
    origin = lambda i, j: i == 0 and j == 0
    last_z = lax.axis_size("gz") - 1
    below = send(edge, lambda i, j: ok(late(i) or (i == 0 and j == last_z), (i + 1, j + 1)))
    above = send(edge, lambda i, j: ok(late(i) or (i == 0 and j == 1), (i + 1, j - 1)))
    up_x = send(up_x, lambda i, j: ok(late(i) or origin(i, j), (i + 1, j)))
    za = []
    for n, turn in enumerate(turns_of(last_z + 1)):
        to = {j: (j + 1) % (last_z + 1) for j in turn}
        to.update({v: k for k, v in to.items()})
        za.append(send(turns_z[n], lambda i, j: ok(j in to and not late(i), (i, to.get(j)))))
    pack = jax.ShapeDtypeStruct((3, NODES, 128), BF16)
    unpack = jax.ShapeDtypeStruct((3, 128, NODES), BF16)
    vmem = pl.BlockSpec(memory_space=pltpu.VMEM)
    block = pltpu.VMEM((2, 5, 12, 2, NODES), F32)
    vol, uz, px, ep, ux, eu = call(
        volume_kernel,
        (field_shape(5), unpack, pack, pack, unpack, unpack),
        10**6,
        in_specs=[hbm] + [vmem] * 5,
        scratch_shapes=[block, pltpu.SemaphoreType.DMA],
    )(reg, st, aux, dh, dl, sw)
    face_buf = [pltpu.VMEM((144, 128), F32)]
    tg, gz, even_x, odd_x = call(
        second_kernel, (field_shape(9), field_shape(9), FACE, FACE), 10**8, scratch_shapes=face_buf
    )(st, tg_first, *za, uz, px, ep)
    early = lambda i: not (late(i) or late(i ^ 1))
    apart = lambda i, j: i < 2 and j in (0, 1, last_z)
    xa_even = send(even_x, lambda i, j: ok(early(i) and not apart(i, j), (i ^ 1, j)))
    x_odd = send(odd_x, lambda i, j: ok(not late(i), (odd_partner(i), j)))
    zb_even = send(even_z, lambda i, j: ok(late(i), (i, j ^ 1)))
    zb_odd = send(odd_z, lambda i, j: ok(late(i), (i, odd_partner(j))))
    tg, gz, even_x = call(
        third_kernel, (field_shape(9), field_shape(9), FACE), 10**8, scratch_shapes=face_buf
    )(st, tg_first, tg, gz, even_x, zb_even, zb_odd, uz, px, ep)
    rest = (vol, st, tg, gz, aux, x_odd, up_x, below, above, dh, dl, sw, ux, eu)
    buffers = [block, block, pltpu.SemaphoreType.DMA((4,))]
    outs = call(
        last_a_kernel, (whole, whole), 10**8, in_specs=[vmem] * 15, out_specs=[hbm, hbm], scratch_shapes=buffers
    )(xa_even, *rest)
    xb_even = send(even_x, lambda i, j: ok(not early(i) or (apart(i, j) and not origin(i, j)), (i ^ 1, j)))
    state_next, reg_next = call(
        last_b_kernel,
        (whole, whole),
        10**8,
        in_specs=[hbm] * 3 + [vmem] * 16,
        out_specs=[hbm, hbm],
        scratch_shapes=buffers + [pltpu.VMEM((5, ROWS, NODES), F32), block, pltpu.SemaphoreType.DMA],
        input_output_aliases={0: 0, 1: 1},
    )(*outs, reg, xa_even, xb_even, *rest)
    return (unrows(state_next), unrows(reg_next))


def solution(mesh):
    spec = P("gx", "gz", None, None, None)

    return jax.shard_map(
        shards,
        mesh=mesh,
        in_specs=(spec, spec, P(), P("gx", "gz", None)),
        out_specs=(spec, spec),
        check_vma=False,
    )
```

```python
import functools
import math

import jax
import jax.numpy as jnp
import numpy as np
from jax import lax
from jax.experimental import pallas as pl
from jax.experimental.pallas import tpu as pltpu
from jax.sharding import PartitionSpec as P


GAMMA = 1.4
VISCOSITY = 0.001
CONDUCT = 0.001 * 1.4 / (0.4 * 0.72)
SCALE_X = 2.0 / 0.2
SCALE_Z = 2.0 / 0.15
TIME_STEP = 0.004
SECTION_A = -0.4178904745
SECTION_B = 0.3792103129
HALF_W = 7.5


ROWS, NODES = (48, 216)
F32, BF16 = (jnp.float32, jnp.bfloat16)


def node_matrix():
    root = math.sqrt(7.0)
    outer = math.sqrt(1.0 / 3.0 + 2.0 * root / 21.0)
    inner = math.sqrt(1.0 / 3.0 - 2.0 * root / 21.0)
    points = np.array([-1.0, -outer, -inner, inner, outer, 1.0])
    barycen = np.array(
        [1.0 / np.prod([points[i] - points[j] for j in range(6) if j != i]) for i in range(6)]
    )
    matrix = np.zeros((6, 6))
    for i in range(6):
        for j in range(6):
            if j != i:
                matrix[i, j] = barycen[j] / barycen[i] / (points[i] - points[j])
        matrix[i, i] = -np.sum(matrix[i])
    return matrix


STRIDE = (36, 6, 1)


def hot(sources, depth):
    rows = lax.broadcasted_iota(jnp.int32, (depth, sources[0].shape[1]), 0)
    found = rows == sources[0]
    for source in sources[1:]:
        found = jnp.logical_or(found, rows == source)
    return jnp.where(found, 1.0, 0.0).astype(BF16)


def slot_lane(first, width):
    lane = lax.broadcasted_iota(jnp.int32, (1, 128), 1) - first
    return jnp.where(jnp.logical_and(lane >= 0, lane < width), lane, -1000)


def pack_table(d, j):
    node = slot_lane(36 * j, 36) * (1 if d == 0 else 6)
    return hot([node, node + 5 * STRIDE[d]], NODES)


def unpack_table(lanes, d, j):
    node = lax.broadcasted_iota(jnp.int32, (1, NODES), 1)
    face = (node % 36) if d == 0 else node // 6
    return hot([jnp.where(lanes.face[d], 36 * j + face, -1)], 128)


def edge_pack_table(j):
    node = 6 * slot_lane(108 + 6 * j, 6)
    return hot([node, node + 5, node + 180, node + 185], NODES)


def edge_unpack_table(lanes, j):
    edge = jnp.logical_and(lanes.face[0], lanes.face[2])
    return hot([jnp.where(edge, 108 + 6 * j + lanes.place[1], -1)], 128)


def swap_table(lanes, d):
    lane = lax.broadcasted_iota(jnp.int32, (1, NODES), 1)
    step = 5 * STRIDE[d]
    return hot(
        [jnp.where(lanes.lo[d], lane + step, jnp.where(lanes.hi[d], lane - step, -1))], NODES
    )


def deriv_table(lanes, matrix, d):
    lane = lax.broadcasted_iota(jnp.int32, (1, NODES), 1)
    base = lane - STRIDE[d] * lanes.place[d]
    rows = lax.broadcasted_iota(jnp.int32, (NODES, NODES), 0) - base
    table = jnp.zeros((NODES, NODES), F32)
    for j in range(6):
        line = jnp.zeros((1, NODES), F32)
        for i in range(6):
            line = jnp.where(lanes.place[d] == i, float(np.float32(matrix[i, j])), line)
        table = jnp.where(rows == STRIDE[d] * j, line, table)
    return table


def halves(value):
    high = value.astype(BF16)
    return (high, (value - high.astype(F32)).astype(BF16))


def dot(a, b):
    return jnp.dot(a, b, preferred_element_type=F32)


def derive(pair, dh, dl):
    return move(pair, dh) + dot(pair[0], dl)


def move(pair, table):
    rows = pair[0].shape[0]
    both = dot(jnp.concatenate(pair, axis=0), table)
    return both[:rows] + both[rows:]


def stack(fields):
    return jnp.concatenate(fields, axis=0)


def rows_of(value, count, size=ROWS):
    return [value[i * size : (i + 1) * size] for i in range(count)]


class Lanes:
    def __init__(self):
        lane = lax.broadcasted_iota(jnp.int32, (1, NODES), 1)
        row = lax.broadcasted_iota(jnp.int32, (ROWS, 1), 0)
        self.a, self.c = (row // 24, row % 2)
        self.k = (row % 24) // 2
        place = (lane // 36, lane // 6 % 6, lane % 6)
        self.place = place
        self.lo = [p == 0 for p in place]
        self.hi = [p == 5 for p in place]
        self.sig = [
            jnp.where(p == 0, 1.0, 0.0) + jnp.where(p == 5, -1.0, 0.0) for p in place
        ]
        self.face = [jnp.logical_or(lo, hi) for lo, hi in zip(self.lo, self.hi)]
        self.ghost_x = jnp.logical_or(
            jnp.logical_and(self.a == 0, self.lo[0]), jnp.logical_and(self.a == 1, self.hi[0])
        )
        self.ghost_z = jnp.logical_or(
            jnp.logical_and(self.c == 0, self.lo[2]), jnp.logical_and(self.c == 1, self.hi[2])
        )


def read_rows(ref, field):
    return stack([ref[a, field].reshape(24, NODES) for a in range(2)])


def load_prims(state_ref):
    rho = state_ref[0]
    inv = 1.0 / rho
    mom = [state_ref[1], state_ref[2], state_ref[3]]
    vel = [m * inv for m in mom]
    energy = state_ref[4]
    pres = (GAMMA - 1.0) * (
        energy - 0.5 * (mom[0] * vel[0] + mom[1] * vel[1] + mom[2] * vel[2])
    )
    return (rho, mom, energy, vel, pres, pres * inv, inv)


def walls_of(mask_ref, lanes):
    spread = jnp.zeros((ROWS, 11), jnp.int32)
    for a in range(2):
        for c in range(2):
            here = jnp.logical_and(lanes.a == a, lanes.c == c)
            spread = jnp.where(here, mask_ref[a, c : c + 1, :], spread)
    column = lax.broadcasted_iota(jnp.int32, (ROWS, 11), 1)
    solid = jnp.where(spread == 1, 1.0, 0.0)
    low = jnp.sum(jnp.where(column == lanes.k - 1, solid, 0.0), axis=1, keepdims=True)
    high = jnp.sum(jnp.where(column == lanes.k, solid, 0.0), axis=1, keepdims=True)
    return (
        jnp.logical_or(low > 0.5, lanes.k == 0),
        jnp.logical_or(high > 0.5, lanes.k == 11),
    )


def scale_y(h_ref, lanes):
    column = lax.broadcasted_iota(jnp.int32, (ROWS, 12), 1)
    own = jnp.where(column == lanes.k, h_ref[0:1, :], 0.0)
    return 2.0 / jnp.sum(own, axis=1, keepdims=True)


def shift(value, by):
    return pltpu.roll(value, by % value.shape[0], 0)


def inner_x(swapped, own, lanes):
    other = stack([swapped[24:48], swapped[0:24]])
    return jnp.where(jnp.logical_and(lanes.face[0], jnp.logical_not(lanes.ghost_x)), other, own)


def inner_z(swapped, own, lanes):
    other = jnp.where(lanes.lo[2], shift(swapped, 1), shift(swapped, -1))
    return jnp.where(jnp.logical_and(lanes.face[2], jnp.logical_not(lanes.ghost_z)), other, own)


def inner_y(swapped, own, lanes, wall_lo, wall_hi, sign):
    other = jnp.where(lanes.lo[1], shift(swapped, 2), shift(swapped, -2))
    solid = jnp.logical_or(
        jnp.logical_and(wall_lo, lanes.lo[1]), jnp.logical_and(wall_hi, lanes.hi[1])
    )
    return jnp.where(lanes.face[1], jnp.where(solid, sign * own, other), own)


def stress(grads):
    gx, gy, gz = grads
    third = (2.0 / 3.0) * VISCOSITY * (gx[0] + gy[1] + gz[2])
    return [
        2.0 * VISCOSITY * gx[0] - third,
        2.0 * VISCOSITY * gy[1] - third,
        2.0 * VISCOSITY * gz[2] - third,
        VISCOSITY * (gx[1] + gy[0]),
        VISCOSITY * (gx[2] + gz[0]),
        VISCOSITY * (gy[2] + gz[1]),
        CONDUCT * gx[3],
        CONDUCT * gy[3],
        CONDUCT * gz[3],
    ]


def add_lift(tg, delta, direction):
    tg = list(tg)
    bulk = (2.0 / 3.0) * VISCOSITY * delta[direction]
    for d in range(3):
        tg[d] = tg[d] - bulk
    tg[direction] = tg[direction] + 2.0 * VISCOSITY * delta[direction]
    for other in range(3):
        if other != direction:
            slot = {1: 3, 2: 4, 3: 5}[direction + other]
            tg[slot] = tg[slot] + VISCOSITY * delta[other]
    tg[6 + direction] = tg[6 + direction] + CONDUCT * delta[3]
    return tg


def flux_of(tg, vel, direction):
    t = [
        (tg[0], tg[3], tg[4]),
        (tg[3], tg[1], tg[5]),
        (tg[4], tg[5], tg[2]),
    ][direction]
    work = vel[0] * t[0] + vel[1] * t[1] + vel[2] * t[2] + tg[6 + direction]
    return [t[0], t[1], t[2], work]


def ghost_lift(flux, vel, delta, direction, lift_direction):
    zero = jnp.zeros_like(delta[0])
    tg = add_lift([zero] * 9, delta, lift_direction)
    change = flux_of(tg, vel, direction)
    return [f + d for f, d in zip(flux, change)]


def pack_faces(fields, table_of):
    total = None
    for j in range(3):
        value = move(halves(stack([fields[3 * s + j] for s in range(3)])), table_of(j))
        total = value if total is None else total + value
    return total


def edge_rows(fields, table_of):
    edges = move(halves(stack([fields[0], fields[3]])), table_of(0))
    first = edges[0:48]
    for j in (1, 2):
        first = first + move(halves(fields[j]), table_of(j))
    return stack([first, edges[48:96]])


def euler(rho, vel, pres, direction):
    normal = vel[direction]
    mass = rho * normal
    square = vel[0] * vel[0] + vel[1] * vel[1] + vel[2] * vel[2]
    energy = pres * (1.0 / (GAMMA - 1.0)) + 0.5 * rho * square
    flux = [mass] + [mass * v for v in vel] + [(energy + pres) * normal]
    flux[1 + direction] = flux[1 + direction] + pres
    state = [rho, rho * vel[0], rho * vel[1], rho * vel[2], energy]
    return (flux, state)


def face_terms(own, out, direction, sig, scale):
    rho, vel, temp = own
    rho_out, vel_out, temp_out = out
    flux, state = euler(rho, vel, rho * temp, direction)
    flux_out, state_out = euler(rho_out, vel_out, rho_out * temp_out, direction)
    speed = jnp.maximum(
        jnp.abs(vel[direction]) + jnp.sqrt(GAMMA * temp),
        jnp.abs(vel_out[direction]) + jnp.sqrt(GAMMA * temp_out),
    )
    speed = speed * jnp.abs(sig)
    return [
        (HALF_W * scale) * (sig * (fo - fi) + speed * (so - si))
        for fi, fo, si, so in zip(flux, flux_out, state, state_out)
    ]


def period_of(size):
    return 32 if size % 32 == 0 else size


def sends_late():
    period = period_of(lax.axis_size("gx"))
    return lax.rem(lax.axis_index("gx"), period) == period - 1


def is_device(gx, gz):
    return jnp.logical_and(lax.axis_index("gx") == gx, lax.axis_index("gz") == gz)


def hears_late():
    first = lax.rem(lax.axis_index("gx"), period_of(lax.axis_size("gx"))) == 0
    return jnp.logical_or(first, is_device(1, 0))


def ends_late():
    period = period_of(lax.axis_size("gx"))
    pair = lax.rem(lax.axis_index("gx"), period) >= period - 2
    last = lax.axis_size("gz") - 1
    near = [is_device(0, 0)] + [is_device(i, j) for i in (0, 1) for j in (1, last)]
    return functools.reduce(jnp.logical_or, near, pair)


def parity_of(axis):
    return lax.rem(lax.axis_index(axis), 2) == 0


def first_kernel(state_hbm, mask_hbm, h_hbm, st_ref, aux_ref, dh_ref, dl_ref, sw_ref, tg_ref,
                 even_ref, odd_ref, turn_1, turn_2, turn_3, edge_ref, upper_ref,
                 uz_ref, px_ref, ep_ref, ux_ref, eu_ref, state_buf, mask_buf, h_buf, face_buf, sems):
    copies = [
        pltpu.make_async_copy(src, dst, sems.at[i])
        for i, (src, dst) in enumerate(
            ((state_hbm, state_buf), (mask_hbm, mask_buf), (h_hbm, h_buf))
        )
    ]
    for copy in copies:
        copy.start()
    lanes = Lanes()
    for d in range(3):
        sw_ref[d] = swap_table(lanes, d)
    matrix = node_matrix()
    for d in range(3):
        high, low = halves(deriv_table(lanes, matrix, d))
        dh_ref[d] = high
        dl_ref[d] = low
    for j in range(3):
        uz_ref[j] = unpack_table(lanes, 2, j)
        px_ref[j] = pack_table(0, j)
        ep_ref[j] = edge_pack_table(j)
        ux_ref[j] = unpack_table(lanes, 0, j)
        eu_ref[j] = edge_unpack_table(lanes, j)
    for copy in copies:
        copy.wait()
    for i in range(5):
        st_ref[i] = read_rows(state_buf, i)
    rho, _, _, vel, _, temp, _ = load_prims(st_ref)
    wall_lo, wall_hi = walls_of(mask_buf, lanes)
    sy = scale_y(h_buf, lanes)
    slot = lax.broadcasted_iota(jnp.int32, (ROWS, 128), 1)
    aux_ref[...] = jnp.where(
        slot == 0,
        jnp.where(wall_lo, 1.0, 0.0),
        jnp.where(slot == 1, jnp.where(wall_hi, 1.0, 0.0), sy),
    )
    own = vel + [temp]
    keep = jnp.logical_and(lanes.ghost_x, lanes.ghost_z)
    edges = edge_rows([jnp.where(keep, f, 0.0) for f in own], lambda j: ep_ref[j])
    edge_ref[...] = stack([edges[24:48], edges[72:96]])
    pair = halves(stack(own))
    scales = (SCALE_X, sy, SCALE_Z)
    grads = []
    for d in range(3):
        slope = rows_of(derive(pair, dh_ref[d], dl_ref[d]), 4)
        swapped = rows_of(move(pair, sw_ref[d]), 4)
        grad = []
        for i in range(4):
            if d == 0:
                out = inner_x(swapped[i], own[i], lanes)
            elif d == 2:
                out = inner_z(swapped[i], own[i], lanes)
            else:
                sign = 1.0 if i == 3 else -1.0
                out = inner_y(swapped[i], own[i], lanes, wall_lo, wall_hi, sign)
            grad.append(scales[d] * (slope[i] + (HALF_W * lanes.sig[d]) * (own[i] - out)))
        grads.append(grad)
    tg = stress(grads)
    for i in range(9):
        tg_ref[i] = tg[i]
    fields = [rho] + own + flux_of(tg, vel, 0)
    fields = [jnp.where(lanes.hi[0], f[24:48], 0.0) for f in fields]
    upper_ref[...] = pack_faces(fields, lambda j: px_ref[j])
    fields = [rho] + own + flux_of(tg, vel, 2)
    fields = [jnp.where(lanes.ghost_z, f, 0.0) for f in fields]
    face_buf[...] = pack_faces(fields, lambda j: pack_table(2, j))
    down = face_buf[pl.ds(0, 72, stride=2), :]
    up = face_buf[pl.ds(1, 72, stride=2), :]
    even = parity_of("gz")
    even_ref[...] = jnp.where(even, up, down)
    odd_ref[...] = jnp.where(even, down, up)
    for ref, turn in zip((turn_1, turn_2, turn_3), turns_of(lax.axis_size("gz"))):
        ref[...] = jnp.where(among(lax.axis_index("gz"), turn), up, down)


def aux_of(aux_ref):
    return (aux_ref[:, 0:1] > 0.5, aux_ref[:, 1:2] > 0.5, aux_ref[:, 2:3])


def volume(reg_hbm, state_ref, aux_ref, dh_ref, dl_ref, sw_ref, out_ref, reg_buf, sem):
    copy = pltpu.make_async_copy(reg_hbm, reg_buf, sem)
    copy.start()
    lanes = Lanes()
    rho, mom, energy, vel, pres, temp, inv = load_prims(state_ref)
    wall_lo, wall_hi, sy = aux_of(aux_ref)
    scales = (SCALE_X, sy, SCALE_Z)
    spec = energy * inv
    common = halves(stack([rho] + vel + [pres, spec] + mom + [energy]))
    swap_pair = halves(stack([rho] + vel + [temp]))
    others = vel + [spec]
    dens = mom + [energy]
    own = [rho] + vel + [temp]
    total = [None] * 5
    for d in range(3):
        normal = vel[d]
        mine = [pres * normal] + [normal * o for o in others] + [normal * m for m in dens]
        base = rows_of(derive(common, dh_ref[d], dl_ref[d]), 10)
        rest = rows_of(derive(halves(stack(mine)), dh_ref[d], dl_ref[d]), 9)
        d_rho, d_pres, d_work = (base[0], base[4], rest[0])
        d_others = base[1:4] + [base[5]]
        d_dens = base[6:10]
        d_norm, d_mass = (base[1 + d], base[6 + d])
        mass = mom[d]
        parts = [0.5 * (rho * d_norm + normal * d_rho + d_mass)]
        for m in range(4):
            value = 0.25 * (
                rest[5 + m]
                + rho * rest[1 + m]
                + normal * d_dens[m]
                + others[m] * (d_mass + rho * d_norm + normal * d_rho)
                + mass * d_others[m]
            )
            if m == d:
                value = value + d_pres
            if m == 3:
                value = value + 0.5 * (pres * d_norm + normal * d_pres + d_work)
            parts.append(value)
        swapped = rows_of(move(swap_pair, sw_ref[d]), 5)
        outs = []
        for i in range(5):
            if d == 0:
                outs.append(inner_x(swapped[i], own[i], lanes))
            elif d == 2:
                outs.append(inner_z(swapped[i], own[i], lanes))
            else:
                sign = -1.0 if i in (1, 2, 3) else 1.0
                outs.append(inner_y(swapped[i], own[i], lanes, wall_lo, wall_hi, sign))
        faces = face_terms(
            (rho, vel, temp), (outs[0], outs[1:4], outs[4]), d, lanes.sig[d], scales[d]
        )
        for i in range(5):
            value = faces[i] - scales[d] * parts[i]
            total[i] = value if d == 0 else total[i] + value
    copy.wait()
    for i in range(5):
        out_ref[i] = SECTION_A * read_rows(reg_buf, i) + TIME_STEP * total[i]


def starts_late():
    return jnp.logical_or(sends_late(), is_device(0, 0))


def volume_kernel(reg_hbm, state_ref, aux_ref, dh_ref, dl_ref, sw_ref, out_ref, reg_buf, sem):
    @pl.when(jnp.logical_not(starts_late()))
    def _():
        volume(reg_hbm, state_ref, aux_ref, dh_ref, dl_ref, sw_ref, out_ref, reg_buf, sem)


def sides_of(from_even, from_odd, axis):
    even = parity_of(axis)
    return (jnp.where(even, from_odd, from_even), jnp.where(even, from_even, from_odd))


def unpack_faces(pair, table_ref, keep):
    fields = [None] * 9
    for j in range(3):
        for s, value in enumerate(rows_of(move(pair, table_ref[j]), 3)):
            fields[3 * s + j] = jnp.where(keep, value, 0.0)
    return fields


def complete_z(lanes, state_ref, tg_ref, lower, upper, uz_ref, px_ref, ep_ref, face_buf):
    rho, _, _, vel, _, temp, _ = load_prims(state_ref)
    own = vel + [temp]
    face_buf[pl.ds(0, 72, stride=2), :] = lower
    face_buf[pl.ds(1, 72, stride=2), :] = upper
    ghost = unpack_faces(halves(face_buf[...]), uz_ref, lanes.ghost_z)
    weight = jnp.where(lanes.ghost_z, (SCALE_Z * HALF_W) * lanes.sig[2], 0.0)
    delta = [weight * (o - g) for o, g in zip(own, ghost[1:5])]
    tg = add_lift([tg_ref[i] for i in range(9)], delta, 2)
    flux = ghost_lift(ghost[5:9], ghost[1:4], delta, 2, 2)
    fields = [rho] + own + flux_of(tg, vel, 0)
    fields = [jnp.where(lanes.ghost_x, f, 0.0) for f in fields]
    total = pack_faces(fields, lambda j: px_ref[j])
    edges = edge_rows([jnp.where(lanes.ghost_x, g, 0.0) for g in ghost[1:5]], lambda j: ep_ref[j])
    total = total + stack([edges, jnp.zeros((ROWS, 128), F32)])
    down = stack([total[48 * s : 48 * s + 24] for s in range(3)])
    up = stack([total[48 * s + 24 : 48 * s + 48] for s in range(3)])
    return (own, tg, ghost[:5] + flux, up, down)


def second_kernel(state_ref, tg_ref, turn_1, turn_2, turn_3, uz_ref, px_ref, ep_ref,
                  tgo_ref, gz_ref, even_out, odd_out, face_buf):
    @pl.when(jnp.logical_not(sends_late()))
    def _():
        lower, upper = (jnp.zeros((72, 128), F32), jnp.zeros((72, 128), F32))
        for ref, turn in zip((turn_1, turn_2, turn_3), turns_of(lax.axis_size("gz"))):
            above = among(lax.axis_index("gz"), turn)
            upper = upper + jnp.where(above, ref[...], 0.0)
            lower = lower + jnp.where(above, 0.0, ref[...])
        _, tg, ghost, up, down = complete_z(Lanes(), state_ref, tg_ref, lower, upper, uz_ref, px_ref, ep_ref, face_buf)
        for i in range(9):
            tgo_ref[i] = tg[i]
            gz_ref[i] = ghost[i]
        even = parity_of("gx")
        even_out[...] = jnp.where(even, up, down)
        odd_out[...] = jnp.where(even, down, up)


def third_kernel(state_ref, tg_first_ref, tg_ref, gz_ref, mine_ref, even_ref, odd_ref,
                 uz_ref, px_ref, ep_ref, tgo_ref, gzo_ref, even_out, face_buf):
    late = sends_late()

    @pl.when(late)
    def _():
        lanes = Lanes()
        lower, upper = sides_of(even_ref[...], odd_ref[...], "gz")
        _, tg, ghost, up, down = complete_z(
            lanes, state_ref, tg_first_ref, lower, upper, uz_ref, px_ref, ep_ref, face_buf
        )
        for i in range(9):
            tgo_ref[i] = tg[i]
            gzo_ref[i] = ghost[i]
        even_out[...] = jnp.where(parity_of("gx"), up, down)

    @pl.when(jnp.logical_not(late))
    def _():
        tgo_ref[...] = tg_ref[...]
        gzo_ref[...] = gz_ref[...]
        even_out[...] = mine_ref[...]


def finish(from_even, vol_ref, state_ref, tg_ref, gz_ref, aux_ref, odd_ref, up_ref,
           below_ref, above_ref, dh_ref, dl_ref, sw_ref, ux_ref, eu_ref,
           state_hbm, reg_hbm, state_out, reg_out, sems):
    lanes = Lanes()
    rho, mom, energy, vel, _, temp, _ = load_prims(state_ref)
    wall_lo, wall_hi, sy = aux_of(aux_ref)
    scales = (SCALE_X, sy, SCALE_Z)
    own = vel + [temp]
    lower, upper = sides_of(from_even, odd_ref[...], "gx")
    lower = lower + up_ref[...]
    late = hears_late()
    row = lax.broadcasted_iota(jnp.int32, (48, 128), 0)
    slot = lax.broadcasted_iota(jnp.int32, (48, 128), 1)
    direct = jnp.where(row % 2 == 0, shift(below_ref[...], -1), shift(above_ref[...], 1))
    edge_slot = jnp.where(late, slot, 0) >= 108
    lower = stack([jnp.where(edge_slot, direct, lower[0:48]), lower[48:72]])
    pair = halves(
        stack([side[24 * s : 24 * s + 24] for s in range(3) for side in (lower, upper)])
    )
    ghost_x = unpack_faces(pair, ux_ref, lanes.ghost_x)
    edge = [rows_of(move(pair, eu_ref[j]), 3) for j in range(3)]
    edge = [edge[0][0], edge[1][0], edge[2][0], edge[0][1]]
    ghost_z = [gz_ref[i] for i in range(9)]
    weight = jnp.where(lanes.ghost_x, (SCALE_X * HALF_W) * lanes.sig[0], 0.0)
    delta = [weight * (o - g) for o, g in zip(own, ghost_x[1:5])]
    tg = add_lift([tg_ref[i] for i in range(9)], delta, 0)
    flux_x = ghost_lift(ghost_x[5:9], ghost_x[1:4], delta, 0, 0)
    weight = jnp.where(lanes.ghost_z, weight, 0.0)
    edge_delta = [weight * (g - e) for g, e in zip(ghost_z[1:5], edge)]
    flux_z = ghost_lift(ghost_z[5:9], ghost_z[1:4], edge_delta, 2, 0)
    weight = jnp.where(lanes.ghost_z, (SCALE_Z * HALF_W) * lanes.sig[2], 0.0)
    weight = jnp.where(jnp.logical_and(lanes.ghost_x, jnp.where(late, lanes.a, 1) == 0), weight, 0.0)
    edge_delta = [weight * (g - e) for g, e in zip(ghost_x[1:5], edge)]
    flux_x = ghost_lift(flux_x, ghost_x[1:4], edge_delta, 0, 2)
    total = [0.0] * 5
    for d, ghost, keep in ((0, ghost_x, lanes.ghost_x), (2, ghost_z, lanes.ghost_z)):
        out = [jnp.where(keep, g, o) for g, o in zip(ghost[:5], [rho] + own)]
        faces = face_terms(
            (rho, vel, temp), (out[0], out[1:4], out[4]), d, lanes.sig[d], scales[d]
        )
        total = [t + f for t, f in zip(total, faces)]
    pairs = []
    for d in range(3):
        flux = flux_of(tg, vel, d)
        pairs.append([halves(f) for f in flux])
        swapped = rows_of(move([stack(list(v)) for v in zip(*pairs[d])], sw_ref[d]), 4)
        for i in range(4):
            if d == 0:
                out = jnp.where(lanes.ghost_x, flux_x[i], inner_x(swapped[i], flux[i], lanes))
            elif d == 2:
                out = jnp.where(lanes.ghost_z, flux_z[i], inner_z(swapped[i], flux[i], lanes))
            else:
                out = inner_y(swapped[i], flux[i], lanes, wall_lo, wall_hi, 1.0)
            total[i + 1] = total[i + 1] + (scales[d] * HALF_W * lanes.sig[d]) * (flux[i] - out)
    fields = [rho] + mom + [energy]
    copies = []
    for a in range(2):
        part = slice(24 * a, 24 * a + 24)
        mine = [t[part] for t in total]
        for d in range(3):
            pair = [stack([f[part] for f in v]) for v in zip(*pairs[d])]
            slope = rows_of(derive(pair, dh_ref[d], dl_ref[d]), 4, 24)
            scale = sy[part] if d == 1 else scales[d]
            for i in range(4):
                mine[i + 1] = mine[i + 1] + scale * slope[i]
        for i in range(5):
            reg = vol_ref[i][part] + TIME_STEP * mine[i]
            reg_out[a, i] = reg.reshape(12, 2, NODES)
            state_out[a, i] = (fields[i][part] + SECTION_B * reg).reshape(12, 2, NODES)
        copies += [
            pltpu.make_async_copy(reg_out.at[a], reg_hbm.at[a], sems.at[2 * a]),
            pltpu.make_async_copy(state_out.at[a], state_hbm.at[a], sems.at[2 * a + 1]),
        ]
        for copy in copies[2 * a :]:
            copy.start()
    for copy in copies:
        copy.wait()


def last_a_kernel(even_ref, vol_ref, *refs):
    @pl.when(jnp.logical_not(ends_late()))
    def _():
        finish(even_ref[...], vol_ref, *refs)


def last_b_kernel(state_in, reg_in, register_hbm, even_a_ref, even_b_ref, vol_ref, state_ref, tg_ref, gz_ref,
                  aux_ref, odd_ref, up_ref, below_ref, above_ref, dh_ref, dl_ref, sw_ref, *refs):
    vol_buf, reg_buf, sem = refs[-3:]

    @pl.when(ends_late())
    def _():
        @pl.when(starts_late())
        def _():
            volume(register_hbm, state_ref, aux_ref, dh_ref, dl_ref, sw_ref, vol_buf, reg_buf, sem)

        @pl.when(jnp.logical_not(starts_late()))
        def _():
            vol_buf[...] = vol_ref[...]

        finish(
            even_a_ref[...] + even_b_ref[...], vol_buf, state_ref, tg_ref, gz_ref, aux_ref, odd_ref,
            up_ref, below_ref, above_ref, dh_ref, dl_ref, sw_ref, *refs[:-3],
        )


def field_shape(count):
    return jax.ShapeDtypeStruct((count, ROWS, NODES), F32)


LIMIT = 20 * 1024 * 1024
FACE = jax.ShapeDtypeStruct((72, 128), F32)


def call(kernel, outs, flops, **more):
    return pl.pallas_call(
        kernel,
        out_shape=outs,
        compiler_params=pltpu.CompilerParams(vmem_limit_bytes=LIMIT),
        cost_estimate=pl.CostEstimate(flops=flops, bytes_accessed=2_000_000, transcendentals=0),
        **more,
    )


def send(value, partner):
    nx, nz = (lax.axis_size("gx"), lax.axis_size("gz"))
    pairs = []
    for i in range(nx):
        for j in range(nz):
            to = partner(i, j)
            if to is not None:
                pairs.append((i * nz + j, (to[0] % nx) * nz + to[1] % nz))
    return lax.ppermute(value, ("gx", "gz"), pairs)


def odd_partner(i):
    return i + 1 if i % 2 else i - 1


def turns_of(size):
    return {8: ((1, 3, 6), (2, 4, 7), (0, 5)), 4: ((1,), (3,), (0, 2))}[size]


def among(position, members):
    found = position == members[0]
    for member in members[1:]:
        found = jnp.logical_or(found, position == member)
    return found


def shards(state, register, heights, solid_wall_mask):
    h = heights.reshape(1, 12)

    def rows(array):
        return jnp.transpose(array, (0, 2, 3, 1, 4))

    def unrows(array):
        return jnp.transpose(array, (0, 3, 1, 2, 4))

    reg = pltpu.with_memory_space_constraint(rows(register), pltpu.HBM)
    whole = jax.ShapeDtypeStruct((2, 5, 12, 2, NODES), F32)
    table = jax.ShapeDtypeStruct((3, NODES, NODES), BF16)
    aux_shape = jax.ShapeDtypeStruct((ROWS, 128), F32)
    hbm = pl.BlockSpec(memory_space=pltpu.HBM)
    edge_shape = jax.ShapeDtypeStruct((48, 128), F32)
    pack = jax.ShapeDtypeStruct((3, NODES, 128), BF16)
    unpack = jax.ShapeDtypeStruct((3, 128, NODES), BF16)
    st, aux, dh, dl, sw, tg_first, even_z, odd_z, *turns_z, edge, up_x, uz, px, ep, ux, eu = call(
        first_kernel,
        (
            field_shape(5), aux_shape, table, table, table, field_shape(9), *[FACE] * 5, edge_shape, FACE,
            unpack, pack, pack, unpack, unpack,
        ),
        10**8,
        in_specs=[hbm] * 3,
        scratch_shapes=[
            pltpu.VMEM((2, 5, 12, 2, NODES), F32),
            pltpu.VMEM((2, 2, 11), jnp.int32),
            pltpu.VMEM((1, 12), F32),
            pltpu.VMEM((144, 128), F32),
            pltpu.SemaphoreType.DMA((3,)),
        ],
    )(*[pltpu.with_memory_space_constraint(v, pltpu.HBM) for v in (rows(state), solid_wall_mask, h)])
    period = period_of(lax.axis_size("gx"))
    late = lambda i: i % period == period - 1
    ok = lambda flag, to: to if flag else None
    origin = lambda i, j: i == 0 and j == 0
    last_z = lax.axis_size("gz") - 1
    below = send(edge, lambda i, j: ok(late(i) or (i == 0 and j == last_z), (i + 1, j + 1)))
    above = send(edge, lambda i, j: ok(late(i) or (i == 0 and j == 1), (i + 1, j - 1)))
    up_x = send(up_x, lambda i, j: ok(late(i) or origin(i, j), (i + 1, j)))
    za = []
    for n, turn in enumerate(turns_of(last_z + 1)):
        to = {j: (j + 1) % (last_z + 1) for j in turn}
        to.update({v: k for k, v in to.items()})
        za.append(send(turns_z[n], lambda i, j: ok(j in to and not late(i), (i, to.get(j)))))
    vmem = pl.BlockSpec(memory_space=pltpu.VMEM)
    block = pltpu.VMEM((2, 5, 12, 2, NODES), F32)
    vol = call(
        volume_kernel,
        field_shape(5),
        10**6,
        in_specs=[hbm] + [vmem] * 5,
        scratch_shapes=[block, pltpu.SemaphoreType.DMA],
    )(reg, st, aux, dh, dl, sw)
    face_buf = [pltpu.VMEM((144, 128), F32)]
    tg, gz, even_x, odd_x = call(
        second_kernel, (field_shape(9), field_shape(9), FACE, FACE), 10**8, scratch_shapes=face_buf
    )(st, tg_first, *za, uz, px, ep)
    early = lambda i: not (late(i) or late(i ^ 1))
    apart = lambda i, j: i < 2 and j in (0, 1, last_z)
    xa_even = send(even_x, lambda i, j: ok(early(i) and not apart(i, j), (i ^ 1, j)))
    x_odd = send(odd_x, lambda i, j: ok(not late(i), (odd_partner(i), j)))
    zb_even = send(even_z, lambda i, j: ok(late(i), (i, j ^ 1)))
    zb_odd = send(odd_z, lambda i, j: ok(late(i), (i, odd_partner(j))))
    tg, gz, even_x = call(
        third_kernel, (field_shape(9), field_shape(9), FACE), 10**8, scratch_shapes=face_buf
    )(st, tg_first, tg, gz, even_x, zb_even, zb_odd, uz, px, ep)
    rest = (vol, st, tg, gz, aux, x_odd, up_x, below, above, dh, dl, sw, ux, eu)
    buffers = [block, block, pltpu.SemaphoreType.DMA((4,))]
    outs = call(
        last_a_kernel, (whole, whole), 10**8, in_specs=[vmem] * 15, out_specs=[hbm, hbm], scratch_shapes=buffers
    )(xa_even, *rest)
    xb_even = send(even_x, lambda i, j: ok(not early(i) or (apart(i, j) and not origin(i, j)), (i ^ 1, j)))
    state_next, reg_next = call(
        last_b_kernel,
        (whole, whole),
        10**8,
        in_specs=[hbm] * 3 + [vmem] * 16,
        out_specs=[hbm, hbm],
        scratch_shapes=buffers + [pltpu.VMEM((5, ROWS, NODES), F32), block, pltpu.SemaphoreType.DMA],
        input_output_aliases={0: 0, 1: 1},
    )(*outs, reg, xa_even, xb_even, *rest)
    return (unrows(state_next), unrows(reg_next))


def solution(mesh):
    spec = P("gx", "gz", None, None, None)

    return jax.shard_map(
        shards,
        mesh=mesh,
        in_specs=(spec, spec, P(), P("gx", "gz", None)),
        out_specs=(spec, spec),
        check_vma=False,
    )
```

```python
import functools
import math

import jax
import jax.numpy as jnp
import numpy as np
from jax import lax
from jax.experimental import pallas as pl
from jax.experimental.pallas import tpu as pltpu
from jax.sharding import PartitionSpec as P


GAMMA = 1.4
VISCOSITY = 0.001
CONDUCT = 0.001 * 1.4 / (0.4 * 0.72)
SCALE_X = 2.0 / 0.2
SCALE_Z = 2.0 / 0.15
TIME_STEP = 0.004
SECTION_A = -0.4178904745
SECTION_B = 0.3792103129
HALF_W = 7.5


ROWS, NODES = (48, 216)
F32, BF16 = (jnp.float32, jnp.bfloat16)


def node_matrix():
    root = math.sqrt(7.0)
    outer = math.sqrt(1.0 / 3.0 + 2.0 * root / 21.0)
    inner = math.sqrt(1.0 / 3.0 - 2.0 * root / 21.0)
    points = np.array([-1.0, -outer, -inner, inner, outer, 1.0])
    barycen = np.array(
        [1.0 / np.prod([points[i] - points[j] for j in range(6) if j != i]) for i in range(6)]
    )
    matrix = np.zeros((6, 6))
    for i in range(6):
        for j in range(6):
            if j != i:
                matrix[i, j] = barycen[j] / barycen[i] / (points[i] - points[j])
        matrix[i, i] = -np.sum(matrix[i])
    return matrix


STRIDE = (36, 6, 1)


def hot(sources, depth):
    rows = lax.broadcasted_iota(jnp.int32, (depth, sources[0].shape[1]), 0)
    found = rows == sources[0]
    for source in sources[1:]:
        found = jnp.logical_or(found, rows == source)
    return jnp.where(found, 1.0, 0.0).astype(BF16)


def slot_lane(first, width):
    lane = lax.broadcasted_iota(jnp.int32, (1, 128), 1) - first
    return jnp.where(jnp.logical_and(lane >= 0, lane < width), lane, -1000)


def pack_table(d, j):
    node = slot_lane(36 * j, 36) * (1 if d == 0 else 6)
    return hot([node, node + 5 * STRIDE[d]], NODES)


def unpack_table(lanes, d, j):
    node = lax.broadcasted_iota(jnp.int32, (1, NODES), 1)
    face = (node % 36) if d == 0 else node // 6
    return hot([jnp.where(lanes.face[d], 36 * j + face, -1)], 128)


def edge_pack_table(j):
    node = 6 * slot_lane(108 + 6 * j, 6)
    return hot([node, node + 5, node + 180, node + 185], NODES)


def edge_unpack_table(lanes, j):
    edge = jnp.logical_and(lanes.face[0], lanes.face[2])
    return hot([jnp.where(edge, 108 + 6 * j + lanes.place[1], -1)], 128)


def swap_table(lanes, d):
    lane = lax.broadcasted_iota(jnp.int32, (1, NODES), 1)
    step = 5 * STRIDE[d]
    return hot(
        [jnp.where(lanes.lo[d], lane + step, jnp.where(lanes.hi[d], lane - step, -1))], NODES
    )


def deriv_table(lanes, matrix, d):
    lane = lax.broadcasted_iota(jnp.int32, (1, NODES), 1)
    base = lane - STRIDE[d] * lanes.place[d]
    rows = lax.broadcasted_iota(jnp.int32, (NODES, NODES), 0) - base
    table = jnp.zeros((NODES, NODES), F32)
    for j in range(6):
        line = jnp.zeros((1, NODES), F32)
        for i in range(6):
            line = jnp.where(lanes.place[d] == i, float(np.float32(matrix[i, j])), line)
        table = jnp.where(rows == STRIDE[d] * j, line, table)
    return table


def halves(value):
    high = value.astype(BF16)
    return (high, (value - high.astype(F32)).astype(BF16))


def dot(a, b):
    return jnp.dot(a, b, preferred_element_type=F32)


def derive(pair, dh, dl):
    return move(pair, dh) + dot(pair[0], dl)


def move(pair, table):
    rows = pair[0].shape[0]
    both = dot(jnp.concatenate(pair, axis=0), table)
    return both[:rows] + both[rows:]


def stack(fields):
    return jnp.concatenate(fields, axis=0)


def rows_of(value, count, size=ROWS):
    return [value[i * size : (i + 1) * size] for i in range(count)]


class Lanes:
    def __init__(self):
        lane = lax.broadcasted_iota(jnp.int32, (1, NODES), 1)
        row = lax.broadcasted_iota(jnp.int32, (ROWS, 1), 0)
        self.a, self.c = (row // 24, row % 2)
        self.k = (row % 24) // 2
        place = (lane // 36, lane // 6 % 6, lane % 6)
        self.place = place
        self.lo = [p == 0 for p in place]
        self.hi = [p == 5 for p in place]
        self.sig = [
            jnp.where(p == 0, 1.0, 0.0) + jnp.where(p == 5, -1.0, 0.0) for p in place
        ]
        self.face = [jnp.logical_or(lo, hi) for lo, hi in zip(self.lo, self.hi)]
        self.ghost_x = jnp.logical_or(
            jnp.logical_and(self.a == 0, self.lo[0]), jnp.logical_and(self.a == 1, self.hi[0])
        )
        self.ghost_z = jnp.logical_or(
            jnp.logical_and(self.c == 0, self.lo[2]), jnp.logical_and(self.c == 1, self.hi[2])
        )


def read_rows(ref, field):
    return stack([ref[a, field].reshape(24, NODES) for a in range(2)])


def load_prims(state_ref):
    rho = state_ref[0]
    inv = 1.0 / rho
    mom = [state_ref[1], state_ref[2], state_ref[3]]
    vel = [m * inv for m in mom]
    energy = state_ref[4]
    pres = (GAMMA - 1.0) * (
        energy - 0.5 * (mom[0] * vel[0] + mom[1] * vel[1] + mom[2] * vel[2])
    )
    return (rho, mom, energy, vel, pres, pres * inv, inv)


def walls_of(mask_ref, lanes):
    spread = jnp.zeros((ROWS, 11), jnp.int32)
    for a in range(2):
        for c in range(2):
            here = jnp.logical_and(lanes.a == a, lanes.c == c)
            spread = jnp.where(here, mask_ref[a, c : c + 1, :], spread)
    column = lax.broadcasted_iota(jnp.int32, (ROWS, 11), 1)
    solid = jnp.where(spread == 1, 1.0, 0.0)
    low = jnp.sum(jnp.where(column == lanes.k - 1, solid, 0.0), axis=1, keepdims=True)
    high = jnp.sum(jnp.where(column == lanes.k, solid, 0.0), axis=1, keepdims=True)
    return (
        jnp.logical_or(low > 0.5, lanes.k == 0),
        jnp.logical_or(high > 0.5, lanes.k == 11),
    )


def scale_y(h_ref, lanes):
    column = lax.broadcasted_iota(jnp.int32, (ROWS, 12), 1)
    own = jnp.where(column == lanes.k, h_ref[0:1, :], 0.0)
    return 2.0 / jnp.sum(own, axis=1, keepdims=True)


def shift(value, by):
    return pltpu.roll(value, by % value.shape[0], 0)


def inner_x(swapped, own, lanes):
    other = stack([swapped[24:48], swapped[0:24]])
    return jnp.where(jnp.logical_and(lanes.face[0], jnp.logical_not(lanes.ghost_x)), other, own)


def inner_z(swapped, own, lanes):
    other = jnp.where(lanes.lo[2], shift(swapped, 1), shift(swapped, -1))
    return jnp.where(jnp.logical_and(lanes.face[2], jnp.logical_not(lanes.ghost_z)), other, own)


def inner_y(swapped, own, lanes, wall_lo, wall_hi, sign):
    other = jnp.where(lanes.lo[1], shift(swapped, 2), shift(swapped, -2))
    solid = jnp.logical_or(
        jnp.logical_and(wall_lo, lanes.lo[1]), jnp.logical_and(wall_hi, lanes.hi[1])
    )
    return jnp.where(lanes.face[1], jnp.where(solid, sign * own, other), own)


def stress(grads):
    gx, gy, gz = grads
    third = (2.0 / 3.0) * VISCOSITY * (gx[0] + gy[1] + gz[2])
    return [
        2.0 * VISCOSITY * gx[0] - third,
        2.0 * VISCOSITY * gy[1] - third,
        2.0 * VISCOSITY * gz[2] - third,
        VISCOSITY * (gx[1] + gy[0]),
        VISCOSITY * (gx[2] + gz[0]),
        VISCOSITY * (gy[2] + gz[1]),
        CONDUCT * gx[3],
        CONDUCT * gy[3],
        CONDUCT * gz[3],
    ]


def add_lift(tg, delta, direction):
    tg = list(tg)
    bulk = (2.0 / 3.0) * VISCOSITY * delta[direction]
    for d in range(3):
        tg[d] = tg[d] - bulk
    tg[direction] = tg[direction] + 2.0 * VISCOSITY * delta[direction]
    for other in range(3):
        if other != direction:
            slot = {1: 3, 2: 4, 3: 5}[direction + other]
            tg[slot] = tg[slot] + VISCOSITY * delta[other]
    tg[6 + direction] = tg[6 + direction] + CONDUCT * delta[3]
    return tg


def flux_of(tg, vel, direction):
    t = [
        (tg[0], tg[3], tg[4]),
        (tg[3], tg[1], tg[5]),
        (tg[4], tg[5], tg[2]),
    ][direction]
    work = vel[0] * t[0] + vel[1] * t[1] + vel[2] * t[2] + tg[6 + direction]
    return [t[0], t[1], t[2], work]


def ghost_lift(flux, vel, delta, direction, lift_direction):
    zero = jnp.zeros_like(delta[0])
    tg = add_lift([zero] * 9, delta, lift_direction)
    change = flux_of(tg, vel, direction)
    return [f + d for f, d in zip(flux, change)]


def pack_faces(fields, table_of):
    total = None
    for j in range(3):
        value = move(halves(stack([fields[3 * s + j] for s in range(3)])), table_of(j))
        total = value if total is None else total + value
    return total


def edge_rows(fields, table_of):
    edges = move(halves(stack([fields[0], fields[3]])), table_of(0))
    first = edges[0:48]
    for j in (1, 2):
        first = first + move(halves(fields[j]), table_of(j))
    return stack([first, edges[48:96]])


def euler(rho, vel, pres, direction):
    normal = vel[direction]
    mass = rho * normal
    square = vel[0] * vel[0] + vel[1] * vel[1] + vel[2] * vel[2]
    energy = pres * (1.0 / (GAMMA - 1.0)) + 0.5 * rho * square
    flux = [mass] + [mass * v for v in vel] + [(energy + pres) * normal]
    flux[1 + direction] = flux[1 + direction] + pres
    state = [rho, rho * vel[0], rho * vel[1], rho * vel[2], energy]
    return (flux, state)


def face_terms(own, out, direction, sig, scale):
    rho, vel, temp = own
    rho_out, vel_out, temp_out = out
    flux, state = euler(rho, vel, rho * temp, direction)
    flux_out, state_out = euler(rho_out, vel_out, rho_out * temp_out, direction)
    speed = jnp.maximum(
        jnp.abs(vel[direction]) + jnp.sqrt(GAMMA * temp),
        jnp.abs(vel_out[direction]) + jnp.sqrt(GAMMA * temp_out),
    )
    speed = speed * jnp.abs(sig)
    return [
        (HALF_W * scale) * (sig * (fo - fi) + speed * (so - si))
        for fi, fo, si, so in zip(flux, flux_out, state, state_out)
    ]


def period_of(size):
    return 32 if size % 32 == 0 else size


def sends_late():
    period = period_of(lax.axis_size("gx"))
    return lax.rem(lax.axis_index("gx"), period) == period - 1


def is_device(gx, gz):
    return jnp.logical_and(lax.axis_index("gx") == gx, lax.axis_index("gz") == gz)


def hears_late():
    first = lax.rem(lax.axis_index("gx"), period_of(lax.axis_size("gx"))) == 0
    return jnp.logical_or(first, is_device(1, 0))


def ends_late():
    period = period_of(lax.axis_size("gx"))
    pair = lax.rem(lax.axis_index("gx"), period) >= period - 2
    near = [is_device(0, 0)] + [is_device(i, j) for i in (0, 1) for j in (1,)]
    return functools.reduce(jnp.logical_or, near, pair)


def parity_of(axis):
    return lax.rem(lax.axis_index(axis), 2) == 0


def first_kernel(state_hbm, mask_hbm, h_hbm, st_ref, aux_ref, dh_ref, dl_ref, sw_ref, tg_ref,
                 even_ref, odd_ref, turn_1, turn_2, turn_3, edge_ref, upper_ref,
                 uz_ref, px_ref, ep_ref, ux_ref, eu_ref, state_buf, mask_buf, h_buf, face_buf, sems):
    copies = [
        pltpu.make_async_copy(src, dst, sems.at[i])
        for i, (src, dst) in enumerate(
            ((state_hbm, state_buf), (mask_hbm, mask_buf), (h_hbm, h_buf))
        )
    ]
    for copy in copies:
        copy.start()
    lanes = Lanes()
    for d in range(3):
        sw_ref[d] = swap_table(lanes, d)
    matrix = node_matrix()
    for d in range(3):
        high, low = halves(deriv_table(lanes, matrix, d))
        dh_ref[d] = high
        dl_ref[d] = low
    for j in range(3):
        uz_ref[j] = unpack_table(lanes, 2, j)
        px_ref[j] = pack_table(0, j)
        ep_ref[j] = edge_pack_table(j)
        ux_ref[j] = unpack_table(lanes, 0, j)
        eu_ref[j] = edge_unpack_table(lanes, j)
    for copy in copies:
        copy.wait()
    for i in range(5):
        st_ref[i] = read_rows(state_buf, i)
    rho, _, _, vel, _, temp, _ = load_prims(st_ref)
    wall_lo, wall_hi = walls_of(mask_buf, lanes)
    sy = scale_y(h_buf, lanes)
    slot = lax.broadcasted_iota(jnp.int32, (ROWS, 128), 1)
    aux_ref[...] = jnp.where(
        slot == 0,
        jnp.where(wall_lo, 1.0, 0.0),
        jnp.where(slot == 1, jnp.where(wall_hi, 1.0, 0.0), sy),
    )
    own = vel + [temp]
    keep = jnp.logical_and(lanes.ghost_x, lanes.ghost_z)
    edges = edge_rows([jnp.where(keep, f, 0.0) for f in own], lambda j: ep_ref[j])
    edge_ref[...] = stack([edges[24:48], edges[72:96]])
    pair = halves(stack(own))
    scales = (SCALE_X, sy, SCALE_Z)
    grads = []
    for d in range(3):
        slope = rows_of(derive(pair, dh_ref[d], dl_ref[d]), 4)
        swapped = rows_of(move(pair, sw_ref[d]), 4)
        grad = []
        for i in range(4):
            if d == 0:
                out = inner_x(swapped[i], own[i], lanes)
            elif d == 2:
                out = inner_z(swapped[i], own[i], lanes)
            else:
                sign = 1.0 if i == 3 else -1.0
                out = inner_y(swapped[i], own[i], lanes, wall_lo, wall_hi, sign)
            grad.append(scales[d] * (slope[i] + (HALF_W * lanes.sig[d]) * (own[i] - out)))
        grads.append(grad)
    tg = stress(grads)
    for i in range(9):
        tg_ref[i] = tg[i]
    fields = [rho] + own + flux_of(tg, vel, 0)
    fields = [jnp.where(lanes.hi[0], f[24:48], 0.0) for f in fields]
    upper_ref[...] = pack_faces(fields, lambda j: px_ref[j])
    fields = [rho] + own + flux_of(tg, vel, 2)
    fields = [jnp.where(lanes.ghost_z, f, 0.0) for f in fields]
    face_buf[...] = pack_faces(fields, lambda j: pack_table(2, j))
    down = face_buf[pl.ds(0, 72, stride=2), :]
    up = face_buf[pl.ds(1, 72, stride=2), :]
    even = parity_of("gz")
    even_ref[...] = jnp.where(even, up, down)
    odd_ref[...] = jnp.where(even, down, up)
    for ref, turn in zip((turn_1, turn_2, turn_3), turns_of(lax.axis_size("gz"))):
        ref[...] = jnp.where(among(lax.axis_index("gz"), turn), up, down)


def aux_of(aux_ref):
    return (aux_ref[:, 0:1] > 0.5, aux_ref[:, 1:2] > 0.5, aux_ref[:, 2:3])


def volume(reg_hbm, state_ref, aux_ref, dh_ref, dl_ref, sw_ref, out_ref, reg_buf, sem):
    copy = pltpu.make_async_copy(reg_hbm, reg_buf, sem)
    copy.start()
    lanes = Lanes()
    rho, mom, energy, vel, pres, temp, inv = load_prims(state_ref)
    wall_lo, wall_hi, sy = aux_of(aux_ref)
    scales = (SCALE_X, sy, SCALE_Z)
    spec = energy * inv
    common = halves(stack([rho] + vel + [pres, spec] + mom + [energy]))
    swap_pair = halves(stack([rho] + vel + [temp]))
    others = vel + [spec]
    dens = mom + [energy]
    own = [rho] + vel + [temp]
    total = [None] * 5
    for d in range(3):
        normal = vel[d]
        mine = [pres * normal] + [normal * o for o in others] + [normal * m for m in dens]
        base = rows_of(derive(common, dh_ref[d], dl_ref[d]), 10)
        rest = rows_of(derive(halves(stack(mine)), dh_ref[d], dl_ref[d]), 9)
        d_rho, d_pres, d_work = (base[0], base[4], rest[0])
        d_others = base[1:4] + [base[5]]
        d_dens = base[6:10]
        d_norm, d_mass = (base[1 + d], base[6 + d])
        mass = mom[d]
        parts = [0.5 * (rho * d_norm + normal * d_rho + d_mass)]
        for m in range(4):
            value = 0.25 * (
                rest[5 + m]
                + rho * rest[1 + m]
                + normal * d_dens[m]
                + others[m] * (d_mass + rho * d_norm + normal * d_rho)
                + mass * d_others[m]
            )
            if m == d:
                value = value + d_pres
            if m == 3:
                value = value + 0.5 * (pres * d_norm + normal * d_pres + d_work)
            parts.append(value)
        swapped = rows_of(move(swap_pair, sw_ref[d]), 5)
        outs = []
        for i in range(5):
            if d == 0:
                outs.append(inner_x(swapped[i], own[i], lanes))
            elif d == 2:
                outs.append(inner_z(swapped[i], own[i], lanes))
            else:
                sign = -1.0 if i in (1, 2, 3) else 1.0
                outs.append(inner_y(swapped[i], own[i], lanes, wall_lo, wall_hi, sign))
        faces = face_terms(
            (rho, vel, temp), (outs[0], outs[1:4], outs[4]), d, lanes.sig[d], scales[d]
        )
        for i in range(5):
            value = faces[i] - scales[d] * parts[i]
            total[i] = value if d == 0 else total[i] + value
    copy.wait()
    for i in range(5):
        out_ref[i] = SECTION_A * read_rows(reg_buf, i) + TIME_STEP * total[i]


def starts_late():
    return jnp.logical_or(sends_late(), is_device(0, 0))


def volume_kernel(reg_hbm, state_ref, aux_ref, dh_ref, dl_ref, sw_ref, out_ref, reg_buf, sem):
    @pl.when(jnp.logical_not(starts_late()))
    def _():
        volume(reg_hbm, state_ref, aux_ref, dh_ref, dl_ref, sw_ref, out_ref, reg_buf, sem)


def sides_of(from_even, from_odd, axis):
    even = parity_of(axis)
    return (jnp.where(even, from_odd, from_even), jnp.where(even, from_even, from_odd))


def unpack_faces(pair, table_ref, keep):
    fields = [None] * 9
    for j in range(3):
        for s, value in enumerate(rows_of(move(pair, table_ref[j]), 3)):
            fields[3 * s + j] = jnp.where(keep, value, 0.0)
    return fields


def complete_z(lanes, state_ref, tg_ref, lower, upper, uz_ref, px_ref, ep_ref, face_buf):
    rho, _, _, vel, _, temp, _ = load_prims(state_ref)
    own = vel + [temp]
    face_buf[pl.ds(0, 72, stride=2), :] = lower
    face_buf[pl.ds(1, 72, stride=2), :] = upper
    ghost = unpack_faces(halves(face_buf[...]), uz_ref, lanes.ghost_z)
    weight = jnp.where(lanes.ghost_z, (SCALE_Z * HALF_W) * lanes.sig[2], 0.0)
    delta = [weight * (o - g) for o, g in zip(own, ghost[1:5])]
    tg = add_lift([tg_ref[i] for i in range(9)], delta, 2)
    flux = ghost_lift(ghost[5:9], ghost[1:4], delta, 2, 2)
    fields = [rho] + own + flux_of(tg, vel, 0)
    fields = [jnp.where(lanes.ghost_x, f, 0.0) for f in fields]
    total = pack_faces(fields, lambda j: px_ref[j])
    edges = edge_rows([jnp.where(lanes.ghost_x, g, 0.0) for g in ghost[1:5]], lambda j: ep_ref[j])
    total = total + stack([edges, jnp.zeros((ROWS, 128), F32)])
    down = stack([total[48 * s : 48 * s + 24] for s in range(3)])
    up = stack([total[48 * s + 24 : 48 * s + 48] for s in range(3)])
    return (own, tg, ghost[:5] + flux, up, down)


def second_kernel(state_ref, tg_ref, turn_1, turn_2, turn_3, uz_ref, px_ref, ep_ref,
                  tgo_ref, gz_ref, even_out, odd_out, face_buf):
    @pl.when(jnp.logical_not(sends_late()))
    def _():
        lower, upper = (jnp.zeros((72, 128), F32), jnp.zeros((72, 128), F32))
        for ref, turn in zip((turn_1, turn_2, turn_3), turns_of(lax.axis_size("gz"))):
            above = among(lax.axis_index("gz"), turn)
            upper = upper + jnp.where(above, ref[...], 0.0)
            lower = lower + jnp.where(above, 0.0, ref[...])
        _, tg, ghost, up, down = complete_z(Lanes(), state_ref, tg_ref, lower, upper, uz_ref, px_ref, ep_ref, face_buf)
        for i in range(9):
            tgo_ref[i] = tg[i]
            gz_ref[i] = ghost[i]
        even = parity_of("gx")
        even_out[...] = jnp.where(even, up, down)
        odd_out[...] = jnp.where(even, down, up)


def third_kernel(state_ref, tg_first_ref, tg_ref, gz_ref, mine_ref, even_ref, odd_ref,
                 uz_ref, px_ref, ep_ref, tgo_ref, gzo_ref, even_out, face_buf):
    late = sends_late()

    @pl.when(late)
    def _():
        lanes = Lanes()
        lower, upper = sides_of(even_ref[...], odd_ref[...], "gz")
        _, tg, ghost, up, down = complete_z(
            lanes, state_ref, tg_first_ref, lower, upper, uz_ref, px_ref, ep_ref, face_buf
        )
        for i in range(9):
            tgo_ref[i] = tg[i]
            gzo_ref[i] = ghost[i]
        even_out[...] = jnp.where(parity_of("gx"), up, down)

    @pl.when(jnp.logical_not(late))
    def _():
        tgo_ref[...] = tg_ref[...]
        gzo_ref[...] = gz_ref[...]
        even_out[...] = mine_ref[...]


def finish(from_even, vol_ref, state_ref, tg_ref, gz_ref, aux_ref, odd_ref, up_ref,
           below_ref, above_ref, dh_ref, dl_ref, sw_ref, ux_ref, eu_ref,
           state_hbm, reg_hbm, state_out, reg_out, sems):
    lanes = Lanes()
    rho, mom, energy, vel, _, temp, _ = load_prims(state_ref)
    wall_lo, wall_hi, sy = aux_of(aux_ref)
    scales = (SCALE_X, sy, SCALE_Z)
    own = vel + [temp]
    lower, upper = sides_of(from_even, odd_ref[...], "gx")
    lower = lower + up_ref[...]
    late = hears_late()
    row = lax.broadcasted_iota(jnp.int32, (48, 128), 0)
    slot = lax.broadcasted_iota(jnp.int32, (48, 128), 1)
    direct = jnp.where(row % 2 == 0, shift(below_ref[...], -1), shift(above_ref[...], 1))
    edge_slot = jnp.where(late, slot, 0) >= 108
    lower = stack([jnp.where(edge_slot, direct, lower[0:48]), lower[48:72]])
    pair = halves(
        stack([side[24 * s : 24 * s + 24] for s in range(3) for side in (lower, upper)])
    )
    ghost_x = unpack_faces(pair, ux_ref, lanes.ghost_x)
    edge = [rows_of(move(pair, eu_ref[j]), 3) for j in range(3)]
    edge = [edge[0][0], edge[1][0], edge[2][0], edge[0][1]]
    ghost_z = [gz_ref[i] for i in range(9)]
    weight = jnp.where(lanes.ghost_x, (SCALE_X * HALF_W) * lanes.sig[0], 0.0)
    delta = [weight * (o - g) for o, g in zip(own, ghost_x[1:5])]
    tg = add_lift([tg_ref[i] for i in range(9)], delta, 0)
    flux_x = ghost_lift(ghost_x[5:9], ghost_x[1:4], delta, 0, 0)
    weight = jnp.where(lanes.ghost_z, weight, 0.0)
    edge_delta = [weight * (g - e) for g, e in zip(ghost_z[1:5], edge)]
    flux_z = ghost_lift(ghost_z[5:9], ghost_z[1:4], edge_delta, 2, 0)
    weight = jnp.where(lanes.ghost_z, (SCALE_Z * HALF_W) * lanes.sig[2], 0.0)
    weight = jnp.where(jnp.logical_and(lanes.ghost_x, jnp.where(late, lanes.a, 1) == 0), weight, 0.0)
    edge_delta = [weight * (g - e) for g, e in zip(ghost_x[1:5], edge)]
    flux_x = ghost_lift(flux_x, ghost_x[1:4], edge_delta, 0, 2)
    total = [0.0] * 5
    for d, ghost, keep in ((0, ghost_x, lanes.ghost_x), (2, ghost_z, lanes.ghost_z)):
        out = [jnp.where(keep, g, o) for g, o in zip(ghost[:5], [rho] + own)]
        faces = face_terms(
            (rho, vel, temp), (out[0], out[1:4], out[4]), d, lanes.sig[d], scales[d]
        )
        total = [t + f for t, f in zip(total, faces)]
    pairs = []
    for d in range(3):
        flux = flux_of(tg, vel, d)
        pairs.append([halves(f) for f in flux])
        swapped = rows_of(move([stack(list(v)) for v in zip(*pairs[d])], sw_ref[d]), 4)
        for i in range(4):
            if d == 0:
                out = jnp.where(lanes.ghost_x, flux_x[i], inner_x(swapped[i], flux[i], lanes))
            elif d == 2:
                out = jnp.where(lanes.ghost_z, flux_z[i], inner_z(swapped[i], flux[i], lanes))
            else:
                out = inner_y(swapped[i], flux[i], lanes, wall_lo, wall_hi, 1.0)
            total[i + 1] = total[i + 1] + (scales[d] * HALF_W * lanes.sig[d]) * (flux[i] - out)
    fields = [rho] + mom + [energy]
    copies = []
    for a in range(2):
        part = slice(24 * a, 24 * a + 24)
        mine = [t[part] for t in total]
        for d in range(3):
            pair = [stack([f[part] for f in v]) for v in zip(*pairs[d])]
            slope = rows_of(derive(pair, dh_ref[d], dl_ref[d]), 4, 24)
            scale = sy[part] if d == 1 else scales[d]
            for i in range(4):
                mine[i + 1] = mine[i + 1] + scale * slope[i]
        for i in range(5):
            reg = vol_ref[i][part] + TIME_STEP * mine[i]
            reg_out[a, i] = reg.reshape(12, 2, NODES)
            state_out[a, i] = (fields[i][part] + SECTION_B * reg).reshape(12, 2, NODES)
        copies += [
            pltpu.make_async_copy(reg_out.at[a], reg_hbm.at[a], sems.at[2 * a]),
            pltpu.make_async_copy(state_out.at[a], state_hbm.at[a], sems.at[2 * a + 1]),
        ]
        for copy in copies[2 * a :]:
            copy.start()
    for copy in copies:
        copy.wait()


def last_a_kernel(even_ref, vol_ref, *refs):
    @pl.when(jnp.logical_not(ends_late()))
    def _():
        finish(even_ref[...], vol_ref, *refs)


def last_b_kernel(state_in, reg_in, register_hbm, even_a_ref, even_b_ref, vol_ref, state_ref, tg_ref, gz_ref,
                  aux_ref, odd_ref, up_ref, below_ref, above_ref, dh_ref, dl_ref, sw_ref, *refs):
    vol_buf, reg_buf, sem = refs[-3:]

    @pl.when(ends_late())
    def _():
        @pl.when(starts_late())
        def _():
            volume(register_hbm, state_ref, aux_ref, dh_ref, dl_ref, sw_ref, vol_buf, reg_buf, sem)

        @pl.when(jnp.logical_not(starts_late()))
        def _():
            vol_buf[...] = vol_ref[...]

        finish(
            even_a_ref[...] + even_b_ref[...], vol_buf, state_ref, tg_ref, gz_ref, aux_ref, odd_ref,
            up_ref, below_ref, above_ref, dh_ref, dl_ref, sw_ref, *refs[:-3],
        )


def field_shape(count):
    return jax.ShapeDtypeStruct((count, ROWS, NODES), F32)


LIMIT = 20 * 1024 * 1024
FACE = jax.ShapeDtypeStruct((72, 128), F32)


def call(kernel, outs, flops, **more):
    return pl.pallas_call(
        kernel,
        out_shape=outs,
        compiler_params=pltpu.CompilerParams(vmem_limit_bytes=LIMIT),
        cost_estimate=pl.CostEstimate(flops=flops, bytes_accessed=2_000_000, transcendentals=0),
        **more,
    )


def send(value, partner):
    nx, nz = (lax.axis_size("gx"), lax.axis_size("gz"))
    pairs = []
    for i in range(nx):
        for j in range(nz):
            to = partner(i, j)
            if to is not None:
                pairs.append((i * nz + j, (to[0] % nx) * nz + to[1] % nz))
    return lax.ppermute(value, ("gx", "gz"), pairs)


def odd_partner(i):
    return i + 1 if i % 2 else i - 1


def turns_of(size):
    return {8: ((1, 3, 6), (2, 4, 7), (0, 5)), 4: ((1,), (3,), (0, 2))}[size]


def among(position, members):
    found = position == members[0]
    for member in members[1:]:
        found = jnp.logical_or(found, position == member)
    return found


def shards(state, register, heights, solid_wall_mask):
    h = heights.reshape(1, 12)

    def rows(array):
        return jnp.transpose(array, (0, 2, 3, 1, 4))

    def unrows(array):
        return jnp.transpose(array, (0, 3, 1, 2, 4))

    reg = pltpu.with_memory_space_constraint(rows(register), pltpu.HBM)
    whole = jax.ShapeDtypeStruct((2, 5, 12, 2, NODES), F32)
    table = jax.ShapeDtypeStruct((3, NODES, NODES), BF16)
    aux_shape = jax.ShapeDtypeStruct((ROWS, 128), F32)
    hbm = pl.BlockSpec(memory_space=pltpu.HBM)
    edge_shape = jax.ShapeDtypeStruct((48, 128), F32)
    pack = jax.ShapeDtypeStruct((3, NODES, 128), BF16)
    unpack = jax.ShapeDtypeStruct((3, 128, NODES), BF16)
    st, aux, dh, dl, sw, tg_first, even_z, odd_z, *turns_z, edge, up_x, uz, px, ep, ux, eu = call(
        first_kernel,
        (
            field_shape(5), aux_shape, table, table, table, field_shape(9), *[FACE] * 5, edge_shape, FACE,
            unpack, pack, pack, unpack, unpack,
        ),
        10**8,
        in_specs=[hbm] * 3,
        scratch_shapes=[
            pltpu.VMEM((2, 5, 12, 2, NODES), F32),
            pltpu.VMEM((2, 2, 11), jnp.int32),
            pltpu.VMEM((1, 12), F32),
            pltpu.VMEM((144, 128), F32),
            pltpu.SemaphoreType.DMA((3,)),
        ],
    )(*[pltpu.with_memory_space_constraint(v, pltpu.HBM) for v in (rows(state), solid_wall_mask, h)])
    period = period_of(lax.axis_size("gx"))
    late = lambda i: i % period == period - 1
    ok = lambda flag, to: to if flag else None
    origin = lambda i, j: i == 0 and j == 0
    last_z = lax.axis_size("gz") - 1
    below = send(edge, lambda i, j: ok(late(i) or (i == 0 and j == last_z), (i + 1, j + 1)))
    above = send(edge, lambda i, j: ok(late(i) or (i == 0 and j == 1), (i + 1, j - 1)))
    up_x = send(up_x, lambda i, j: ok(late(i) or origin(i, j), (i + 1, j)))
    za = []
    for n, turn in enumerate(turns_of(last_z + 1)):
        to = {j: (j + 1) % (last_z + 1) for j in turn}
        to.update({v: k for k, v in to.items()})
        za.append(send(turns_z[n], lambda i, j: ok(j in to and not late(i), (i, to.get(j)))))
    vmem = pl.BlockSpec(memory_space=pltpu.VMEM)
    block = pltpu.VMEM((2, 5, 12, 2, NODES), F32)
    vol = call(
        volume_kernel,
        field_shape(5),
        10**6,
        in_specs=[hbm] + [vmem] * 5,
        scratch_shapes=[block, pltpu.SemaphoreType.DMA],
    )(reg, st, aux, dh, dl, sw)
    face_buf = [pltpu.VMEM((144, 128), F32)]
    tg, gz, even_x, odd_x = call(
        second_kernel, (field_shape(9), field_shape(9), FACE, FACE), 10**8, scratch_shapes=face_buf
    )(st, tg_first, *za, uz, px, ep)
    early = lambda i: not (late(i) or late(i ^ 1))
    apart = lambda i, j: i < 2 and j in (0, 1)
    xa_even = send(even_x, lambda i, j: ok(early(i) and not apart(i, j), (i ^ 1, j)))
    x_odd = send(odd_x, lambda i, j: ok(not late(i), (odd_partner(i), j)))
    zb_even = send(even_z, lambda i, j: ok(late(i), (i, j ^ 1)))
    zb_odd = send(odd_z, lambda i, j: ok(late(i), (i, odd_partner(j))))
    tg, gz, even_x = call(
        third_kernel, (field_shape(9), field_shape(9), FACE), 10**8, scratch_shapes=face_buf
    )(st, tg_first, tg, gz, even_x, zb_even, zb_odd, uz, px, ep)
    rest = (vol, st, tg, gz, aux, x_odd, up_x, below, above, dh, dl, sw, ux, eu)
    buffers = [block, block, pltpu.SemaphoreType.DMA((4,))]
    outs = call(
        last_a_kernel, (whole, whole), 10**8, in_specs=[vmem] * 15, out_specs=[hbm, hbm], scratch_shapes=buffers
    )(xa_even, *rest)
    xb_even = send(even_x, lambda i, j: ok(not early(i) or (apart(i, j) and not origin(i, j)), (i ^ 1, j)))
    state_next, reg_next = call(
        last_b_kernel,
        (whole, whole),
        10**8,
        in_specs=[hbm] * 3 + [vmem] * 16,
        out_specs=[hbm, hbm],
        scratch_shapes=buffers + [pltpu.VMEM((5, ROWS, NODES), F32), block, pltpu.SemaphoreType.DMA],
        input_output_aliases={0: 0, 1: 1},
    )(*outs, reg, xa_even, xb_even, *rest)
    return (unrows(state_next), unrows(reg_next))


def solution(mesh):
    spec = P("gx", "gz", None, None, None)

    return jax.shard_map(
        shards,
        mesh=mesh,
        in_specs=(spec, spec, P(), P("gx", "gz", None)),
        out_specs=(spec, spec),
        check_vma=False,
    )
```
